512 devices in a mesh: rows: 64 (over z, y_hi, x), cols: 8 (over y_lo, core).
Axes of the slice: x: 4, y: 8 (y_hi: 2, y_lo: 4; y = y_hi * 4 + y_lo), z: 8, core: 2. Of those that a mesh axis runs over, the one named last changes fastest.
Arguments:
- pair_map: bfloat16 [32, 512, 8192], P(None, 'cols', 'rows'), may hold values from -44 to 44
- conv_in: bfloat16 [32, 288], replicated, may hold values from -0.375 to 0.375
- embed_weight: bfloat16 [2048, 256], replicated, may hold values from -0.125 to 0.125
- qkv_weight: bfloat16 [256, 768], replicated, may hold values from -0.5 to 0.5
- key_bias: bfloat16 [1024, 64, 8], P('rows', 'cols'), may hold values from -4 to 260
- out_weight: bfloat16 [256, 256], replicated, may hold values from -0.375 to 0.375
- unpatch: bfloat16 [256, 2048], replicated, may hold values from -0.375 to 0.375
- conv_out: bfloat16 [32, 288], replicated, may hold values from -0.375 to 0.375
Outputs:
- trunk_out: bfloat16 [32, 512, 8192], P(None, 'cols', 'rows')
The draws below stay inside these ranges and needn't reach their ends.
All inputs are finite; a program needn't handle non-finite values.
Results may differ from the reference program's by a relative error of at most 0.014.
Values may be sent and summed in bfloat16 or wider, within the bound.
No kernel may reach another device: no remote copies, remote signals or barrier semaphores. Data moves between devices by JAX's collectives and lax.ppermute only.
A program may use at most 128 MiB of HBM per device.

```python
import jax
import jax.numpy as jnp
from jax import lax

C = 32
PATCH = 8
D = 256
HEADS = 8
HEAD_DIM = 32
ROWS_DEV = 128
COLS_DEV = 64
LENGTH = 8192
SLAB = 512
PROWS = 1024
PCOLS = 64


def draw_pair_map(key, part):
    base_key = jax.random.fold_in(key, 23)
    map_shape = (C, SLAB, LENGTH)
    col_place = jnp.arange(SLAB) % COLS_DEV
    row_place = jnp.arange(LENGTH) % ROWS_DEV
    col_edge = jnp.logical_or(col_place == 0, col_place == COLS_DEV - 1)
    row_edge = jnp.logical_or(row_place == 0, row_place == ROWS_DEV - 1)
    corner = jnp.logical_and(col_edge[:, None], row_edge[None, :])[None, :, :]
    spread = jnp.clip(jax.random.normal(base_key, map_shape, jnp.float32), -6.0, 6.0)
    peak = jnp.where(spread >= 0.0, 1.0, -1.0) * (28.0 + 4.0 * jnp.minimum(jnp.abs(spread), 4.0))
    return jnp.where(corner, peak, spread).astype(jnp.bfloat16)


def draw_key_bias(key, part):
    base_key = jax.random.fold_in(key, 11)
    key_list = jax.random.split(base_key, 5)
    bias_shape = (PROWS, PCOLS, HEADS)
    pair_count = PCOLS * HEADS
    row_index = jnp.arange(PROWS)[:, None]
    background = jax.random.uniform(key_list[0], (PROWS, pair_count), jnp.float32, 0.0, 0.9)
    spike_row = jax.random.randint(key_list[4], (pair_count,), 0, PROWS)
    values = jnp.where(row_index == spike_row[None, :], 8.0, background)
    return values.reshape(bias_shape).astype(jnp.bfloat16)


def noise(key, dims, width, bound, dtype=jnp.bfloat16):
    entries = jax.random.normal(key, dims, jnp.float32) * width
    return jnp.minimum(jnp.maximum(entries, -bound), bound).astype(dtype)


def setup_inputs(seed: int = 0) -> dict:
    key_of = jax.random.split(jax.random.key(seed), 9)
    pair_map = draw_pair_map(jax.random.fold_in(key_of[8], 71), 0)
    conv_in = noise(key_of[1], (C, 9 * C), (9 * C) ** -0.5, 0.375)
    embed_weight = noise(key_of[2], (C * PATCH * PATCH, D), (C * PATCH * PATCH) ** -0.5, 0.125)
    qkv_weight = noise(key_of[3], (D, 3 * D), (D // 2) ** -0.5, 0.5)
    key_bias = draw_key_bias(jax.random.fold_in(key_of[8], 71), 0)
    out_weight = noise(key_of[5], (D, D), D ** -0.5, 0.375)
    unpatch = noise(key_of[6], (D, C * PATCH * PATCH), D ** -0.5, 0.375)
    conv_out = noise(key_of[7], (C, 9 * C), (9 * C) ** -0.5, 0.375)
    return dict(pair_map=pair_map, conv_in=conv_in, embed_weight=embed_weight, qkv_weight=qkv_weight, key_bias=key_bias, out_weight=out_weight, unpatch=unpatch, conv_out=conv_out)


epsilon = 1e-05

def convolve(source_map, weight):
    kernel = weight.astype(jnp.float32).reshape(C, 3, 3, C).transpose(0, 3, 1, 2)
    result = lax.conv_general_dilated(source_map.astype(jnp.float32)[None], kernel, (1, 1), ((1, 1), (1, 1)), dimension_numbers=('NCHW', 'OIHW', 'NCHW'), precision=lax.Precision.HIGHEST)
    return result[0]

def layer_norm(tokens):
    values = tokens.astype(jnp.float32)
    row_mean = lax.optimization_barrier(jnp.mean(values, axis=1, keepdims=True))
    centered = values - row_mean
    row_var = lax.optimization_barrier(jnp.mean(centered * centered, axis=1, keepdims=True))
    return (centered * lax.rsqrt(row_var + epsilon)).astype(jnp.bfloat16)

def attend(qkv_rows, bias_row):
    seq_length = qkv_rows.shape[0]
    block_rows = min(512, seq_length)
    queries = qkv_rows[:, :HEAD_DIM]
    key_rows = qkv_rows[:, HEAD_DIM:2 * HEAD_DIM]
    value_rows = qkv_rows[:, 2 * HEAD_DIM:]
    key_shift = bias_row.astype(jnp.float32)[None, :]
    score_scale = HEAD_DIM ** (-0.5)

    def one_block(query_block):
        scores = jnp.dot(query_block, key_rows.T, preferred_element_type=jnp.float32) * score_scale + key_shift
        row_peak = lax.optimization_barrier(jnp.max(scores, axis=1, keepdims=True))
        weights = jnp.exp(scores - row_peak)
        soft_weights = (weights / lax.optimization_barrier(jnp.sum(weights, axis=1, keepdims=True))).astype(jnp.bfloat16)
        return jnp.dot(soft_weights, value_rows, preferred_element_type=jnp.float32).astype(jnp.bfloat16)
    result = lax.map(one_block, queries.reshape(seq_length // block_rows, block_rows, HEAD_DIM))
    return result.reshape(seq_length, HEAD_DIM)

def attend_pair(pair_item):
    return attend(pair_item[0], pair_item[1])

def reference(pair_map, conv_in, embed_weight, qkv_weight, key_bias, out_weight, unpatch, conv_out):
    first_conv = convolve(pair_map, conv_in)
    mixed_map = (pair_map.astype(jnp.float32) + jax.nn.silu(first_conv)).astype(jnp.bfloat16)
    patches = mixed_map.reshape(C, PCOLS, PATCH, PROWS, PATCH).transpose(3, 1, 0, 2, 4).reshape(PROWS * PCOLS, C * PATCH * PATCH)
    tokens = jnp.dot(patches, embed_weight, preferred_element_type=jnp.float32).astype(jnp.bfloat16)
    normed = layer_norm(tokens)
    projected = jnp.dot(normed, qkv_weight, preferred_element_type=jnp.float32).astype(jnp.bfloat16)
    pair_items = projected.reshape(PROWS, PCOLS, 3, HEADS, HEAD_DIM).transpose(1, 3, 0, 2, 4).reshape(PCOLS * HEADS, PROWS, 3 * HEAD_DIM)
    biases = key_bias.transpose(1, 2, 0).reshape(PCOLS * HEADS, PROWS)
    attended = lax.map(attend_pair, (pair_items, biases))
    attended = attended.reshape(PCOLS, HEADS, PROWS, HEAD_DIM).transpose(2, 0, 1, 3).reshape(PROWS * PCOLS, D)
    updated = (tokens.astype(jnp.float32) + jnp.dot(attended, out_weight, preferred_element_type=jnp.float32)).astype(jnp.bfloat16)
    expanded = jnp.dot(updated, unpatch, preferred_element_type=jnp.float32)
    expanded = expanded.reshape(PROWS, PCOLS, C, PATCH, PATCH).transpose(2, 1, 3, 0, 4).reshape(C, SLAB, LENGTH)
    merged = (mixed_map.astype(jnp.float32) + expanded).astype(jnp.bfloat16)
    second_conv = convolve(merged, conv_out)
    return (merged.astype(jnp.float32) + second_conv).astype(jnp.bfloat16)
```

```python
import jax
import jax.numpy as jnp
from jax import lax
from jax.experimental import pallas as pl
from jax.experimental.pallas import tpu as pltpu
from jax.sharding import PartitionSpec as P

C = 32
PATCH = 8
D = 256
HEADS = 8
HEAD_DIM = 32
W = 64
L = 128
PC = W // PATCH
PR = L // PATCH
GROUPS = 64
SEQ = GROUPS * PR
QUAD = 4
epsilon = 1e-05

f32 = jnp.float32
bf16 = jnp.bfloat16
NT = (((1,), (1,)), ((), ()))


def iota(shape, dim):
    return lax.broadcasted_iota(jnp.int32, shape, dim)


def one_hot(condition):
    return jnp.where(condition, 1.0, 0.0).astype(bf16)


def column_edges(slab_of, edges_ref):
    lane = iota((C, L), 1)
    edges = jnp.zeros((C, L), f32)
    for w in range(W):
        slab = slab_of(w)
        first = pltpu.roll(slab, w, 1) if w else slab
        last = pltpu.roll(slab, (W + w + 1) % L, 1) if (W + w + 1) % L else slab
        edges = jnp.where(lane == w, first, edges)
        edges = jnp.where(lane == W + w, last, edges)
    edges_ref[...] = edges.astype(bf16)


def turn_kernel(x_ref, turned_ref, edges_ref, turned_f32):
    turned_f32[...] = jnp.swapaxes(x_ref[...].astype(f32), 0, 1)
    turned_ref[...] = turned_f32[...].astype(bf16)
    column_edges(lambda w: turned_f32[w], edges_ref)


def weights_kernel(embed_ref, unpatch_ref, embed_out, unpatch_out):
    for source, target in ((embed_ref[...].astype(f32), embed_out), (unpatch_ref[...].astype(f32).T, unpatch_out)):
        turned = jnp.swapaxes(source.reshape(C, PATCH * PATCH, D), 0, 1)
        for i in range(PATCH):
            for j in range(PATCH):
                target[i, j * C : (j + 1) * C, :] = turned[j * PATCH + i].astype(bf16)


def fill_taps(map_ref, low_row, high_row, low_col, high_col, taps):
    lane = iota((C, L), 1)
    row_low = low_row[...].astype(f32)
    row_high = high_row[...].astype(f32)
    below = [low_col[n].astype(f32) for n in range(4)]
    above = [high_col[n].astype(f32) for n in range(4)]
    for w in range(-1, W + 1):
        if w < 0:
            slab, left, right = below[1], below[2][:, L - 1 : L], below[3][:, W - 1 : W]
        elif w == W:
            slab, left, right = above[0], above[2][:, W : W + 1], above[3][:, 0:1]
        else:
            slab = map_ref[w].astype(f32)
            left, right = row_low[:, W + w : W + w + 1], row_high[:, w : w + 1]
        taps[w + 1, 0:C, :] = jnp.where(lane == 0, left, pltpu.roll(slab, 1, 1)).astype(bf16)
        taps[w + 1, C : 2 * C, :] = slab.astype(bf16)
        taps[w + 1, 2 * C : 3 * C, :] = jnp.where(lane == L - 1, right, pltpu.roll(slab, L - 1, 1)).astype(bf16)


def banded(weight):
    weight = weight.astype(f32)
    rows = []
    for i in range(QUAD):
        pieces = [weight]
        if i:
            pieces.insert(0, jnp.zeros((C, 3 * C * i), f32))
        if i < QUAD - 1:
            pieces.append(jnp.zeros((C, 3 * C * (QUAD - 1 - i)), f32))
        rows.append(jnp.concatenate(pieces, axis=1))
    return jnp.concatenate(rows, axis=0).astype(bf16)


def conv_quad(band, taps, group):
    window = taps[group * QUAD : group * QUAD + QUAD + 2].reshape((QUAD + 2) * 3 * C, L)
    return jnp.dot(band, window, preferred_element_type=f32)


def front_kernel(
    map_ref, low_row, high_row, low_col, high_col, conv_ref, embed_ref, qkv_ref, bias_ref,
    mixed_ref, tokens_ref, packed_ref, taps, gathered,
):
    fill_taps(map_ref, low_row, high_row, low_col, high_col, taps)
    band = banded(conv_ref[...])
    row = iota((L, L), 0)
    select = one_hot(iota((L, L), 1) == (row % PR) * PATCH + row // PR)
    for p in range(PC):
        for half in range(PATCH // QUAD):
            group = p * (PATCH // QUAD) + half
            value = conv_quad(band, taps, group)
            value = value / (1.0 + jnp.exp(-value))
            for i in range(QUAD):
                w = group * QUAD + i
                cell = taps[w + 1, C : 2 * C, :].astype(f32) + value[i * C : (i + 1) * C]
                mixed_ref[w] = cell.astype(bf16)
        block = mixed_ref[p * PATCH : (p + 1) * PATCH].reshape(PATCH * C, L)
        sorted_cells = lax.dot_general(select, block, NT, preferred_element_type=f32).astype(bf16)
        for i in range(PATCH):
            gathered[p * PR : (p + 1) * PR, i * D : (i + 1) * D] = sorted_cells[i * PR : (i + 1) * PR]
    tokens = jnp.dot(
        gathered[...], embed_ref[...].reshape(PATCH * D, D), preferred_element_type=f32
    ).astype(bf16)
    tokens_ref[...] = tokens
    values = tokens.astype(f32)
    centered = values - jnp.mean(values, axis=1, keepdims=True)
    spread = jnp.mean(centered * centered, axis=1, keepdims=True)
    normed = (centered * lax.rsqrt(spread + epsilon)).astype(bf16)
    projected = jnp.dot(normed, qkv_ref[...], preferred_element_type=f32)
    bias = bias_ref[...].astype(f32)
    filler = jnp.zeros((PR * PC, L - 3 * HEAD_DIM - 1), f32)
    for h in range(HEADS):
        pieces = [projected[:, g * D + h * HEAD_DIM : g * D + (h + 1) * HEAD_DIM] for g in range(3)]
        tile = jnp.concatenate(pieces + [bias[:, h : h + 1], filler], axis=1).astype(bf16)
        for p in range(PC):
            packed_ref[p * HEADS + h] = tile[p * PR : (p + 1) * PR]


def attention_kernel(packed_ref, out_ref, rows_f32):
    rows = packed_ref[...].reshape(SEQ, L)
    lane = iota((SEQ, L), 1)
    wide = rows.astype(f32)
    rows_f32[...] = pltpu.roll(jnp.where(lane < HEAD_DIM, wide, 0.0), HEAD_DIM, 1)
    pick = one_hot((iota((8, L), 1) == 3 * HEAD_DIM))
    bias = lax.dot_general(pick, rows, NT, preferred_element_type=f32)[0:1]
    values = jnp.where((lane >= 2 * HEAD_DIM) & (lane < 3 * HEAD_DIM), wide, 0.0)
    scale = HEAD_DIM ** (-0.5)
    total = jnp.zeros((SEQ // 4, L), f32)
    for quarter in range(4):
        queries = rows_f32[pl.ds(quarter, SEQ // 4, stride=4), :].astype(bf16)
        scores = lax.dot_general(queries, rows, NT, preferred_element_type=f32) * scale + bias
        peak = jnp.max(scores, axis=1, keepdims=True)
        weights = jnp.exp(scores - peak)
        share = (weights * (1.0 / jnp.sum(weights, axis=1, keepdims=True))).astype(bf16)
        shift = (quarter * HEAD_DIM - 2 * HEAD_DIM) % L
        placed = (pltpu.roll(values, shift, 1) if shift else values).astype(bf16)
        total = total + jnp.dot(share, placed, preferred_element_type=f32)
    out_ref[...] = total.astype(bf16)


def merge_kernel(
    returned_ref, tokens_ref, out_weight_ref, unpatch_ref, mixed_ref,
    merged_ref, edges_ref, returned_f32, rows_f32, repeated,
):
    returned_f32[...] = returned_ref[...].astype(f32)
    for low in range(4):
        heads = [returned_f32[pl.ds(h * 4 + low, PC, stride=HEADS * 4), :] for h in range(HEADS)]
        for high in range(4):
            line = jnp.concatenate([x[:, high * HEAD_DIM : (high + 1) * HEAD_DIM] for x in heads], axis=1)
            at = (low * 4 + high) * PC
            rows_f32[at : at + PC, :] = line
    place = iota((PR * PC, PR * PC), 0)
    order = one_hot(iota((PR * PC, PR * PC), 1) == (place % PR) * PC + place // PR)
    attended = jnp.dot(order, rows_f32[...].astype(bf16), preferred_element_type=f32).astype(bf16)
    updated = (
        tokens_ref[...].astype(f32) + jnp.dot(attended, out_weight_ref[...], preferred_element_type=f32)
    ).astype(bf16)
    repeat = one_hot(iota((PC * L, PR * PC), 0) // PATCH == iota((PC * L, PR * PC), 1))
    repeated[...] = jnp.dot(repeat, updated, preferred_element_type=f32)
    inner = iota((L, D), 0) % PATCH
    for p in range(PC):
        block = repeated[p * L : (p + 1) * L, :]
        grown = jnp.zeros((D, L), f32)
        for i in range(PATCH):
            part = jnp.where(inner == i, block, 0.0).astype(bf16)
            grown = grown + lax.dot_general(unpatch_ref[i], part, NT, preferred_element_type=f32)
        cells = mixed_ref[p * PATCH : (p + 1) * PATCH].astype(f32) + grown.reshape(PATCH, C, L)
        merged_ref[p * PATCH : (p + 1) * PATCH] = cells.astype(bf16)
    column_edges(lambda w: merged_ref[w].astype(f32), edges_ref)


def back_kernel(map_ref, low_row, high_row, low_col, high_col, conv_ref, out_ref, taps, result):
    fill_taps(map_ref, low_row, high_row, low_col, high_col, taps)
    band = banded(conv_ref[...])
    for group in range(W // QUAD):
        value = conv_quad(band, taps, group)
        for i in range(QUAD):
            w = group * QUAD + i
            result[w] = taps[w + 1, C : 2 * C, :].astype(f32) + value[i * C : (i + 1) * C]
    out_ref[...] = jnp.swapaxes(result[...], 0, 1).astype(bf16)


def shape(*dims, dtype=bf16):
    return jax.ShapeDtypeStruct(dims, dtype)


def call(kernel, outs, scratch, *args, flops=0):
    return pl.pallas_call(
        kernel,
        out_shape=outs,
        scratch_shapes=scratch,
        name=kernel.__name__,
        cost_estimate=pl.CostEstimate(flops=flops, transcendentals=0, bytes_accessed=1 << 20),
        compiler_params=pltpu.CompilerParams(vmem_limit_bytes=56 << 20),
    )(*args)


def exchange(block, axis):
    count = lax.axis_size(axis)
    forward = [(i, i + 1) for i in range(count - 1)]
    backward = [(target, source) for source, target in forward]
    return lax.ppermute(block, axis, forward), lax.ppermute(block, axis, backward)


def rims(turned, edges):
    low_row, high_row = exchange(edges, "rows")
    strip = jnp.stack([turned[0], turned[W - 1], low_row, high_row])
    low_col, high_col = exchange(strip, "cols")
    return low_row, high_row, low_col, high_col


def per_device(pair_map, conv_in, embed_weight, qkv_weight, key_bias, out_weight, unpatch, conv_out):
    turned, edges = call(
        turn_kernel, (shape(W, C, L), shape(C, L)), [pltpu.VMEM((W, C, L), f32)], pair_map
    )
    embed_rows, unpatch_rows = call(
        weights_kernel, (shape(PATCH, D, D), shape(PATCH, D, D)), [], embed_weight, unpatch, flops=1 << 32
    )
    bias = key_bias.transpose(1, 0, 2).reshape(PR * PC, HEADS)
    mixed, tokens, packed = call(
        front_kernel,
        (shape(W, C, L), shape(PR * PC, D), shape(GROUPS, PR, L)),
        [pltpu.VMEM((W + 2, 3 * C, L), bf16), pltpu.VMEM((PR * PC, PATCH * D), bf16)],
        turned, *rims(turned, edges), conv_in, embed_rows, qkv_weight, bias,
    )
    arrived = lax.all_to_all(packed, "rows", split_axis=0, concat_axis=0, tiled=True)
    heads_out = call(
        attention_kernel, shape(SEQ // 4, L), [pltpu.VMEM((SEQ, L), f32)], arrived
    )
    returned = lax.all_to_all(
        heads_out.reshape(GROUPS, 4, L), "rows", split_axis=0, concat_axis=0, tiled=True
    ).reshape(GROUPS * 4, L)
    merged, edges = call(
        merge_kernel,
        (shape(W, C, L), shape(C, L)),
        [pltpu.VMEM((GROUPS * 4, L), f32), pltpu.VMEM((PR * PC, D), f32), pltpu.VMEM((PC * L, D), f32)],
        returned, tokens, out_weight, unpatch_rows, mixed,
    )
    return call(
        back_kernel,
        shape(C, W, L),
        [pltpu.VMEM((W + 2, 3 * C, L), bf16), pltpu.VMEM((W, C, L), f32)],
        merged, *rims(merged, edges), conv_out,
    )


def solution(mesh):
    placed = (P(None, "cols", "rows"), P(), P(), P(), P("rows", "cols", None), P(), P(), P())
    return jax.shard_map(
        per_device, mesh=mesh, in_specs=placed, out_specs=P(None, "cols", "rows"), check_vma=False
    )
```

```python
import jax
import jax.numpy as jnp
from jax import lax
from jax.experimental import pallas as pl
from jax.experimental.pallas import tpu as pltpu
from jax.sharding import PartitionSpec as P

C = 32
PATCH = 8
D = 256
HEADS = 8
HEAD_DIM = 32
W = 64
L = 128
PC = W // PATCH
PR = L // PATCH
GROUPS = 64
SEQ = GROUPS * PR
QUAD = 4
epsilon = 1e-05

f32 = jnp.float32
bf16 = jnp.bfloat16
NT = (((1,), (1,)), ((), ()))


def iota(shape, dim):
    return lax.broadcasted_iota(jnp.int32, shape, dim)


def one_hot(condition):
    return jnp.where(condition, 1.0, 0.0).astype(bf16)


def column_edges(slab_of, edges_ref):
    lane = iota((C, L), 1)
    edges = jnp.zeros((C, L), f32)
    for w in range(W):
        slab = slab_of(w)
        first = pltpu.roll(slab, w, 1) if w else slab
        last = pltpu.roll(slab, (W + w + 1) % L, 1) if (W + w + 1) % L else slab
        edges = jnp.where(lane == w, first, edges)
        edges = jnp.where(lane == W + w, last, edges)
    edges_ref[...] = edges.astype(bf16)


def turn_kernel(x_ref, turned_ref, edges_ref, ends_ref, turned_f32):
    turned_f32[...] = jnp.swapaxes(x_ref[...].astype(f32), 0, 1)
    turned_ref[...] = turned_f32[...].astype(bf16)
    ends_ref[0] = turned_ref[0]
    ends_ref[1] = turned_ref[W - 1]
    column_edges(lambda w: turned_f32[w], edges_ref)


def weights_kernel(embed_ref, unpatch_ref, embed_out, unpatch_out):
    for source, target in ((embed_ref[...].astype(f32), embed_out), (unpatch_ref[...].astype(f32).T, unpatch_out)):
        turned = jnp.swapaxes(source.reshape(C, PATCH * PATCH, D), 0, 1)
        for i in range(PATCH):
            for j in range(PATCH):
                target[i, j * C : (j + 1) * C, :] = turned[j * PATCH + i].astype(bf16)


def fill_taps(map_ref, low_row, high_row, low_col, high_col, taps):
    lane = iota((C, L), 1)
    row_low = low_row[...].astype(f32)
    row_high = high_row[...].astype(f32)
    below = [low_col[n].astype(f32) for n in range(4)]
    above = [high_col[n].astype(f32) for n in range(4)]
    for w in range(-1, W + 1):
        if w < 0:
            slab, left, right = below[1], below[2][:, L - 1 : L], below[3][:, W - 1 : W]
        elif w == W:
            slab, left, right = above[0], above[2][:, W : W + 1], above[3][:, 0:1]
        else:
            slab = map_ref[w].astype(f32)
            left, right = row_low[:, W + w : W + w + 1], row_high[:, w : w + 1]
        taps[w + 1, 0:C, :] = jnp.where(lane == 0, left, pltpu.roll(slab, 1, 1)).astype(bf16)
        taps[w + 1, C : 2 * C, :] = slab.astype(bf16)
        taps[w + 1, 2 * C : 3 * C, :] = jnp.where(lane == L - 1, right, pltpu.roll(slab, L - 1, 1)).astype(bf16)


def banded(weight):
    weight = weight.astype(f32)
    rows = []
    for i in range(QUAD):
        pieces = [weight]
        if i:
            pieces.insert(0, jnp.zeros((C, 3 * C * i), f32))
        if i < QUAD - 1:
            pieces.append(jnp.zeros((C, 3 * C * (QUAD - 1 - i)), f32))
        rows.append(jnp.concatenate(pieces, axis=1))
    return jnp.concatenate(rows, axis=0).astype(bf16)


def conv_quad(band, taps, group):
    window = taps[group * QUAD : group * QUAD + QUAD + 2].reshape((QUAD + 2) * 3 * C, L)
    return jnp.dot(band, window, preferred_element_type=f32)


def front_kernel(
    map_ref, low_row, high_row, low_col, high_col, conv_ref, embed_ref, qkv_ref, bias_ref,
    mixed_ref, tokens_ref, packed_ref, taps, gathered,
):
    fill_taps(map_ref, low_row, high_row, low_col, high_col, taps)
    band = banded(conv_ref[...])
    row = iota((L, L), 0)
    select = one_hot(iota((L, L), 1) == (row % PR) * PATCH + row // PR)
    for p in range(PC):
        for half in range(PATCH // QUAD):
            group = p * (PATCH // QUAD) + half
            value = conv_quad(band, taps, group)
            value = value / (1.0 + jnp.exp(-value))
            for i in range(QUAD):
                w = group * QUAD + i
                cell = taps[w + 1, C : 2 * C, :].astype(f32) + value[i * C : (i + 1) * C]
                mixed_ref[w] = cell.astype(bf16)
        block = mixed_ref[p * PATCH : (p + 1) * PATCH].reshape(PATCH * C, L)
        sorted_cells = lax.dot_general(select, block, NT, preferred_element_type=f32).astype(bf16)
        for i in range(PATCH):
            gathered[p * PR : (p + 1) * PR, i * D : (i + 1) * D] = sorted_cells[i * PR : (i + 1) * PR]
    tokens = jnp.dot(
        gathered[...], embed_ref[...].reshape(PATCH * D, D), preferred_element_type=f32
    ).astype(bf16)
    tokens_ref[...] = tokens
    values = tokens.astype(f32)
    centered = values - jnp.mean(values, axis=1, keepdims=True)
    spread = jnp.mean(centered * centered, axis=1, keepdims=True)
    normed = (centered * lax.rsqrt(spread + epsilon)).astype(bf16)
    projected = jnp.dot(normed, qkv_ref[...], preferred_element_type=f32)
    bias = bias_ref[...].astype(f32).reshape(PC * HEADS, PR).T
    filler = jnp.zeros((PR * PC, L - 3 * HEAD_DIM - 1), f32)
    for h in range(HEADS):
        pieces = [projected[:, g * D + h * HEAD_DIM : g * D + (h + 1) * HEAD_DIM] for g in range(3)]
        column = [bias[:, p * HEADS + h : p * HEADS + h + 1] for p in range(PC)]
        tile = jnp.concatenate(pieces + [jnp.concatenate(column, axis=0), filler], axis=1).astype(bf16)
        for p in range(PC):
            packed_ref[p * HEADS + h] = tile[p * PR : (p + 1) * PR]


def attention_kernel(packed_ref, out_ref, rows_f32):
    rows = packed_ref[...].reshape(SEQ, L)
    lane = iota((SEQ, L), 1)
    wide = rows.astype(f32)
    rows_f32[...] = pltpu.roll(jnp.where(lane < HEAD_DIM, wide, 0.0), HEAD_DIM, 1)
    pick = one_hot((iota((8, L), 1) == 3 * HEAD_DIM))
    bias = lax.dot_general(pick, rows, NT, preferred_element_type=f32)[0:1]
    values = jnp.where((lane >= 2 * HEAD_DIM) & (lane < 3 * HEAD_DIM), wide, 0.0)
    scale = HEAD_DIM ** (-0.5)
    total = jnp.zeros((SEQ // 4, L), f32)
    for quarter in range(4):
        queries = rows_f32[pl.ds(quarter, SEQ // 4, stride=4), :].astype(bf16)
        scores = lax.dot_general(queries, rows, NT, preferred_element_type=f32) * scale + bias
        peak = jnp.max(scores, axis=1, keepdims=True)
        weights = jnp.exp(scores - peak)
        share = (weights * (1.0 / jnp.sum(weights, axis=1, keepdims=True))).astype(bf16)
        shift = (quarter * HEAD_DIM - 2 * HEAD_DIM) % L
        placed = (pltpu.roll(values, shift, 1) if shift else values).astype(bf16)
        total = total + jnp.dot(share, placed, preferred_element_type=f32)
    out_ref[...] = total.astype(bf16)


def merge_kernel(
    returned_ref, tokens_ref, out_weight_ref, unpatch_ref, mixed_ref,
    merged_ref, edges_ref, ends_ref, returned_f32, rows_f32, repeated,
):
    returned_f32[...] = returned_ref[...].astype(f32)
    for low in range(4):
        heads = [returned_f32[pl.ds(h * 4 + low, PC, stride=HEADS * 4), :] for h in range(HEADS)]
        for high in range(4):
            line = jnp.concatenate([x[:, high * HEAD_DIM : (high + 1) * HEAD_DIM] for x in heads], axis=1)
            at = (low * 4 + high) * PC
            rows_f32[at : at + PC, :] = line
    place = iota((PR * PC, PR * PC), 0)
    order = one_hot(iota((PR * PC, PR * PC), 1) == (place % PR) * PC + place // PR)
    attended = jnp.dot(order, rows_f32[...].astype(bf16), preferred_element_type=f32).astype(bf16)
    updated = (
        tokens_ref[...].astype(f32) + jnp.dot(attended, out_weight_ref[...], preferred_element_type=f32)
    ).astype(bf16)
    repeat = one_hot(iota((PC * L, PR * PC), 0) // PATCH == iota((PC * L, PR * PC), 1))
    repeated[...] = jnp.dot(repeat, updated, preferred_element_type=f32)
    inner = iota((L, D), 0) % PATCH
    for p in range(PC):
        block = repeated[p * L : (p + 1) * L, :]
        grown = jnp.zeros((D, L), f32)
        for i in range(PATCH):
            part = jnp.where(inner == i, block, 0.0).astype(bf16)
            grown = grown + lax.dot_general(unpatch_ref[i], part, NT, preferred_element_type=f32)
        cells = mixed_ref[p * PATCH : (p + 1) * PATCH].astype(f32) + grown.reshape(PATCH, C, L)
        merged_ref[p * PATCH : (p + 1) * PATCH] = cells.astype(bf16)
    ends_ref[0] = merged_ref[0]
    ends_ref[1] = merged_ref[W - 1]
    column_edges(lambda w: merged_ref[w].astype(f32), edges_ref)


def back_kernel(map_ref, low_row, high_row, low_col, high_col, conv_ref, out_ref, taps, result):
    fill_taps(map_ref, low_row, high_row, low_col, high_col, taps)
    band = banded(conv_ref[...])
    for group in range(W // QUAD):
        value = conv_quad(band, taps, group)
        for i in range(QUAD):
            w = group * QUAD + i
            result[w] = taps[w + 1, C : 2 * C, :].astype(f32) + value[i * C : (i + 1) * C]
    out_ref[...] = jnp.swapaxes(result[...], 0, 1).astype(bf16)


def shape(*dims, dtype=bf16):
    return pltpu.VMEM(dims, dtype)


def call(kernel, outs, scratch, *args, flops=0):
    return pl.pallas_call(
        kernel,
        out_shape=outs,
        in_specs=[pl.BlockSpec(memory_space=pltpu.VMEM)] * len(args),
        scratch_shapes=scratch,
        name=kernel.__name__,
        cost_estimate=pl.CostEstimate(flops=flops, transcendentals=0, bytes_accessed=1 << 20),
        compiler_params=pltpu.CompilerParams(vmem_limit_bytes=24 << 20),
    )(*(pltpu.with_memory_space_constraint(x, pltpu.VMEM) for x in args))


def exchange(block, axis):
    count = lax.axis_size(axis)
    forward = [(i, i + 1) for i in range(count - 1)]
    backward = [(target, source) for source, target in forward]
    return lax.ppermute(block, axis, forward), lax.ppermute(block, axis, backward)


def rims(ends, edges, *ready):
    low_row, high_row, *ready = lax.optimization_barrier((*exchange(edges, "rows"), *ready))
    strip = jnp.concatenate([ends, low_row[None], high_row[None]])
    low_col, high_col = exchange(strip, "cols")
    return low_row, high_row, low_col, high_col, *ready


def per_device(pair_map, conv_in, embed_weight, qkv_weight, key_bias, out_weight, unpatch, conv_out):
    turned, edges, ends = call(
        turn_kernel, (shape(W, C, L), shape(C, L), shape(2, C, L)), [pltpu.VMEM((W, C, L), f32)], pair_map
    )
    embed_rows, unpatch_rows = call(
        weights_kernel, (shape(PATCH, D, D), shape(PATCH, D, D)), [], embed_weight, unpatch, flops=1 << 32
    )
    *borders, embed_rows, unpatch_rows = rims(ends, edges, embed_rows, unpatch_rows)
    mixed, tokens, packed = call(
        front_kernel,
        (shape(W, C, L), shape(PR * PC, D), shape(GROUPS, PR, L)),
        [pltpu.VMEM((W + 2, 3 * C, L), bf16), pltpu.VMEM((PR * PC, PATCH * D), bf16)],
        turned, *borders, conv_in, embed_rows, qkv_weight, key_bias.transpose(1, 2, 0),
    )
    arrived = lax.all_to_all(packed, "rows", split_axis=0, concat_axis=0, tiled=True)
    heads_out = call(
        attention_kernel, shape(SEQ // 4, L), [pltpu.VMEM((SEQ, L), f32)], arrived
    )
    returned = lax.all_to_all(
        heads_out.reshape(GROUPS, 4, L), "rows", split_axis=0, concat_axis=0, tiled=True
    ).reshape(GROUPS * 4, L)
    merged, edges, ends = call(
        merge_kernel,
        (shape(W, C, L), shape(C, L), shape(2, C, L)),
        [pltpu.VMEM((GROUPS * 4, L), f32), pltpu.VMEM((PR * PC, D), f32), pltpu.VMEM((PC * L, D), f32)],
        returned, tokens, out_weight, unpatch_rows, mixed,
    )
    return call(
        back_kernel,
        jax.ShapeDtypeStruct((C, W, L), bf16),
        [pltpu.VMEM((W + 2, 3 * C, L), bf16), pltpu.VMEM((W, C, L), f32)],
        merged, *rims(ends, edges), conv_out,
    )


def solution(mesh):
    placed = (P(None, "cols", "rows"), P(), P(), P(), P("rows", "cols", None), P(), P(), P())
    return jax.shard_map(
        per_device, mesh=mesh, in_specs=placed, out_specs=P(None, "cols", "rows"), check_vma=False
    )
```

```python
import jax
import jax.numpy as jnp
from jax import lax
from jax.experimental import pallas as pl
from jax.experimental.pallas import tpu as pltpu
from jax.sharding import PartitionSpec as P

C = 32
PATCH = 8
D = 256
HEADS = 8
HEAD_DIM = 32
W = 64
L = 128
PC = W // PATCH
PR = L // PATCH
GROUPS = 64
SEQ = GROUPS * PR
OWN = PR * PC
WIDE = OWN + 2 * PC
WINDOW = 8
QUAD = 4
epsilon = 1e-05

f32 = jnp.float32
bf16 = jnp.bfloat16
NT = (((1,), (1,)), ((), ()))


def iota(shape, dim):
    return lax.broadcasted_iota(jnp.int32, shape, dim)


def one_hot(condition):
    return jnp.where(condition, 1.0, 0.0).astype(bf16)


def column_edges(slab_of, edges_ref):
    lane = iota((C, L), 1)
    edges = jnp.zeros((C, L), f32)
    for w in range(W):
        slab = slab_of(w)
        first = pltpu.roll(slab, w, 1) if w else slab
        last = pltpu.roll(slab, (W + w + 1) % L, 1) if (W + w + 1) % L else slab
        edges = jnp.where(lane == w, first, edges)
        edges = jnp.where(lane == W + w, last, edges)
    edges_ref[...] = edges.astype(bf16)


def turn_kernel(x_ref, turned_ref, edges_ref, ends_ref, turned_f32):
    turned_f32[...] = jnp.swapaxes(x_ref[...].astype(f32), 0, 1)
    turned_ref[...] = turned_f32[...].astype(bf16)
    ends_ref[0] = turned_ref[0]
    ends_ref[1] = turned_ref[W - 1]
    column_edges(lambda w: turned_f32[w], edges_ref)


def weights_kernel(embed_ref, unpatch_ref, embed_out, unpatch_out):
    for source, target in ((embed_ref[...].astype(f32), embed_out), (unpatch_ref[...].astype(f32).T, unpatch_out)):
        turned = jnp.swapaxes(source.reshape(C, PATCH * PATCH, D), 0, 1)
        for i in range(PATCH):
            for j in range(PATCH):
                target[i, j * C : (j + 1) * C, :] = turned[j * PATCH + i].astype(bf16)


def fill_taps(map_ref, strip, low_strip, high_strip, taps):
    lane = iota((C, L), 1)
    outer = strip[2].astype(f32)
    below = [low_strip[n].astype(f32) for n in range(3)]
    above = [high_strip[n].astype(f32) for n in range(3)]
    for w in range(-1, W + 1):
        if w < 0:
            slab, left, right = below[1], below[2][:, L - 1 : L], below[2][:, W - 1 : W]
        elif w == W:
            slab, left, right = above[0], above[2][:, W : W + 1], above[2][:, 0:1]
        else:
            slab = map_ref[w].astype(f32)
            left, right = outer[:, W + w : W + w + 1], outer[:, w : w + 1]
        taps[w + 1, 0:C, :] = jnp.where(lane == 0, left, pltpu.roll(slab, 1, 1)).astype(bf16)
        taps[w + 1, C : 2 * C, :] = slab.astype(bf16)
        taps[w + 1, 2 * C : 3 * C, :] = jnp.where(lane == L - 1, right, pltpu.roll(slab, L - 1, 1)).astype(bf16)


def banded(weight):
    weight = weight.astype(f32)
    rows = []
    for i in range(QUAD):
        pieces = [weight]
        if i:
            pieces.insert(0, jnp.zeros((C, 3 * C * i), f32))
        if i < QUAD - 1:
            pieces.append(jnp.zeros((C, 3 * C * (QUAD - 1 - i)), f32))
        rows.append(jnp.concatenate(pieces, axis=1))
    return jnp.concatenate(rows, axis=0).astype(bf16)


def conv_quad(band, taps, group):
    window = taps[group * QUAD : group * QUAD + QUAD + 2].reshape((QUAD + 2) * 3 * C, L)
    return jnp.dot(band, window, preferred_element_type=f32)


def front_kernel(
    map_ref, strip_ref, low_strip, high_strip, conv_ref, embed_ref, qkv_ref, bias_ref,
    mixed_ref, tokens_ref, packed_ref, rim_ref, taps, gathered, tokens_f32, rim_f32,
):
    fill_taps(map_ref, strip_ref, low_strip, high_strip, taps)
    band = banded(conv_ref[...])
    row = iota((L, L), 0)
    select = one_hot(iota((L, L), 1) == (row % PR) * PATCH + row // PR)
    for p in range(PC):
        for half in range(PATCH // QUAD):
            group = p * (PATCH // QUAD) + half
            value = conv_quad(band, taps, group)
            value = value / (1.0 + jnp.exp(-value))
            for i in range(QUAD):
                w = group * QUAD + i
                cell = taps[w + 1, C : 2 * C, :].astype(f32) + value[i * C : (i + 1) * C]
                mixed_ref[w] = cell.astype(bf16)
        block = mixed_ref[p * PATCH : (p + 1) * PATCH].reshape(PATCH * C, L)
        sorted_cells = lax.dot_general(select, block, NT, preferred_element_type=f32).astype(bf16)
        for i in range(PATCH):
            gathered[p * PR : (p + 1) * PR, i * D : (i + 1) * D] = sorted_cells[i * PR : (i + 1) * PR]
    tokens = jnp.dot(
        gathered[...], embed_ref[...].reshape(PATCH * D, D), preferred_element_type=f32
    ).astype(bf16)
    tokens_ref[...] = tokens
    values = tokens.astype(f32)
    for half in range(2):
        tokens_f32[...] = values[:, half * L : (half + 1) * L]
        for n, r in enumerate((0, PR - 1)):
            at = (2 * half + n) * PC
            rim_f32[at : at + PC, :] = tokens_f32[pl.ds(r, PC, stride=PR), :]
    rim_ref[1] = rim_f32[...].astype(bf16)
    column_edges(lambda w: mixed_ref[w].astype(f32), rim_ref.at[0])
    centered = values - jnp.mean(values, axis=1, keepdims=True)
    spread = jnp.mean(centered * centered, axis=1, keepdims=True)
    normed = (centered * lax.rsqrt(spread + epsilon)).astype(bf16)
    projected = jnp.dot(normed, qkv_ref[...], preferred_element_type=f32)
    bias = bias_ref[...].astype(f32).reshape(PC * HEADS, PR).T
    filler = jnp.zeros((PR * PC, L - 3 * HEAD_DIM - 1), f32)
    for h in range(HEADS):
        pieces = [projected[:, g * D + h * HEAD_DIM : g * D + (h + 1) * HEAD_DIM] for g in range(3)]
        column = [bias[:, p * HEADS + h : p * HEADS + h + 1] for p in range(PC)]
        tile = jnp.concatenate(pieces + [jnp.concatenate(column, axis=0), filler], axis=1).astype(bf16)
        for p in range(PC):
            packed_ref[p * HEADS + h] = tile[p * PR : (p + 1) * PR]


def attention_kernel(packed_ref, out_ref, rows_f32, padded, windows):
    rows = packed_ref[...].reshape(SEQ, L)
    lane = iota((SEQ, L), 1)
    wide = rows.astype(f32)
    rows_f32[...] = pltpu.roll(jnp.where(lane < HEAD_DIM, wide, 0.0), HEAD_DIM, 1)
    pick = one_hot((iota((8, L), 1) == 3 * HEAD_DIM))
    bias = lax.dot_general(pick, rows, NT, preferred_element_type=f32)[0:1]
    values = jnp.where((lane >= 2 * HEAD_DIM) & (lane < 3 * HEAD_DIM), wide, 0.0)
    scale = HEAD_DIM ** (-0.5)
    total = jnp.zeros((SEQ // 4, L), f32)
    for quarter in range(4):
        queries = rows_f32[pl.ds(quarter, SEQ // 4, stride=4), :].astype(bf16)
        scores = lax.dot_general(queries, rows, NT, preferred_element_type=f32) * scale + bias
        peak = jnp.max(scores, axis=1, keepdims=True)
        weights = jnp.exp(scores - peak)
        share = (weights * (1.0 / jnp.sum(weights, axis=1, keepdims=True))).astype(bf16)
        shift = (quarter * HEAD_DIM - 2 * HEAD_DIM) % L
        placed = (pltpu.roll(values, shift, 1) if shift else values).astype(bf16)
        total = total + jnp.dot(share, placed, preferred_element_type=f32)
    pad = jnp.zeros((8, L), f32)
    padded[0:8, :] = pad
    padded[8 : 8 + SEQ // 4, :] = total
    padded[8 + SEQ // 4 :, :] = pad
    for n in range(WINDOW):
        start = 7 + min(n, 5)
        windows[pl.ds(n, GROUPS, stride=WINDOW), :] = padded[pl.ds(start, GROUPS, stride=4), :]
    out_ref[...] = windows[...].reshape(GROUPS, WINDOW, L).astype(bf16)


def merge_kernel(
    returned_ref, tokens_ref, low_rim, high_rim, out_weight_ref, unpatch_ref, mixed_ref,
    merged_ref, strip_ref, returned_f32, rows_f32, repeated,
):
    returned_f32[...] = returned_ref[...].astype(f32).reshape(GROUPS * WINDOW, L)
    for n in range(6):
        heads = [
            returned_f32[pl.ds(h * WINDOW + n, PC, stride=HEADS * WINDOW), :] for h in range(HEADS)
        ]
        for high in {0: (3,), 5: (0,)}.get(n, range(4)):
            line = jnp.concatenate([x[:, high * HEAD_DIM : (high + 1) * HEAD_DIM] for x in heads], axis=1)
            at = {0: OWN, 5: OWN + PC}.get(n, ((n - 1) * 4 + high) * PC)
            rows_f32[at : at + PC, :] = line
    place, source = iota((WIDE, WIDE), 0), iota((WIDE, WIDE), 1)
    order = one_hot(source == jnp.where(place < OWN, (place % PR) * PC + place // PR, place))
    attended = jnp.dot(order, rows_f32[...].astype(bf16), preferred_element_type=f32).astype(bf16)
    low, high = low_rim[1].astype(f32), high_rim[1].astype(f32)
    tokens = jnp.concatenate(
        [
            tokens_ref[...].astype(f32),
            jnp.concatenate([low[PC : 2 * PC], low[3 * PC : 4 * PC]], axis=1),
            jnp.concatenate([high[0:PC], high[2 * PC : 3 * PC]], axis=1),
        ],
        axis=0,
    )
    updated = (
        tokens + jnp.dot(attended, out_weight_ref[...], preferred_element_type=f32)
    ).astype(bf16)
    place, source = iota((L, WIDE), 0), iota((L, WIDE), 1)
    spread = one_hot(source == jnp.where(place < W, OWN + PC + place // PATCH, OWN + place // PATCH - PC))
    near = jnp.dot(spread, updated, preferred_element_type=f32)
    after = iota((L, D), 0) < W
    grown = lax.dot_general(
        unpatch_ref[0], jnp.where(after, near, 0.0).astype(bf16), NT, preferred_element_type=f32
    ) + lax.dot_general(
        unpatch_ref[PATCH - 1], jnp.where(after, 0.0, near).astype(bf16), NT, preferred_element_type=f32
    )
    lane = iota((C, L), 1)
    outer = jnp.where(lane < W, high_rim[0].astype(f32), low_rim[0].astype(f32))
    for j in range(PATCH):
        outer = outer + jnp.where(lane % PATCH == j, grown[j * C : (j + 1) * C], 0.0)
    strip_ref[2] = outer.astype(bf16)
    repeat = one_hot(iota((PC * L, WIDE), 0) // PATCH == iota((PC * L, WIDE), 1))
    repeated[...] = jnp.dot(repeat, updated, preferred_element_type=f32)
    inner = iota((L, D), 0) % PATCH
    for p in range(PC):
        block = repeated[p * L : (p + 1) * L, :]
        grown = jnp.zeros((D, L), f32)
        for i in range(PATCH):
            part = jnp.where(inner == i, block, 0.0).astype(bf16)
            grown = grown + lax.dot_general(unpatch_ref[i], part, NT, preferred_element_type=f32)
        cells = mixed_ref[p * PATCH : (p + 1) * PATCH].astype(f32) + grown.reshape(PATCH, C, L)
        merged_ref[p * PATCH : (p + 1) * PATCH] = cells.astype(bf16)
    strip_ref[0] = merged_ref[0]
    strip_ref[1] = merged_ref[W - 1]


def back_kernel(map_ref, strip_ref, low_strip, high_strip, conv_ref, out_ref, taps, result):
    fill_taps(map_ref, strip_ref, low_strip, high_strip, taps)
    band = banded(conv_ref[...])
    for group in range(W // QUAD):
        value = conv_quad(band, taps, group)
        for i in range(QUAD):
            w = group * QUAD + i
            result[w] = taps[w + 1, C : 2 * C, :].astype(f32) + value[i * C : (i + 1) * C]
    out_ref[...] = jnp.swapaxes(result[...], 0, 1).astype(bf16)


def shape(*dims, dtype=bf16):
    return pltpu.VMEM(dims, dtype)


def call(kernel, outs, scratch, *args, flops=0):
    return pl.pallas_call(
        kernel,
        out_shape=outs,
        in_specs=[pl.BlockSpec(memory_space=pltpu.VMEM)] * len(args),
        scratch_shapes=scratch,
        name=kernel.__name__,
        cost_estimate=pl.CostEstimate(flops=flops, transcendentals=0, bytes_accessed=1 << 20),
        compiler_params=pltpu.CompilerParams(vmem_limit_bytes=24 << 20),
    )(*(pltpu.with_memory_space_constraint(x, pltpu.VMEM) for x in args))


def exchange(block, axis):
    count = lax.axis_size(axis)
    forward = [(i, i + 1) for i in range(count - 1)]
    backward = [(target, source) for source, target in forward]
    return lax.ppermute(block, axis, forward), lax.ppermute(block, axis, backward)


def per_device(pair_map, conv_in, embed_weight, qkv_weight, key_bias, out_weight, unpatch, conv_out):
    turned, edges, ends = call(
        turn_kernel, (shape(W, C, L), shape(C, L), shape(2, C, L)), [pltpu.VMEM((W, C, L), f32)], pair_map
    )
    embed_rows, unpatch_rows = call(
        weights_kernel, (shape(PATCH, D, D), shape(PATCH, D, D)), [], embed_weight, unpatch, flops=1 << 32
    )
    low_row, high_row, embed_rows, unpatch_rows = lax.optimization_barrier(
        (*exchange(edges, "rows"), embed_rows, unpatch_rows)
    )
    outer = jnp.where(iota((C, L), 1) < W, high_row, low_row)
    strip = jnp.concatenate([ends, outer[None]])
    mixed, tokens, packed, rim = call(
        front_kernel,
        (shape(W, C, L), shape(OWN, D), shape(GROUPS, PR, L), shape(2, C, L)),
        [
            pltpu.VMEM((W + 2, 3 * C, L), bf16), pltpu.VMEM((OWN, PATCH * D), bf16),
            pltpu.VMEM((OWN, L), f32), pltpu.VMEM((4 * PC, L), f32),
        ],
        turned, strip, *exchange(strip, "cols"), conv_in, embed_rows, qkv_weight, key_bias.transpose(1, 2, 0),
    )
    low_rim, high_rim = exchange(rim, "rows")
    arrived = lax.all_to_all(packed, "rows", split_axis=0, concat_axis=0, tiled=True)
    heads_out = call(
        attention_kernel,
        shape(GROUPS, WINDOW, L),
        [
            pltpu.VMEM((SEQ, L), f32), pltpu.VMEM((SEQ // 4 + 16, L), f32),
            pltpu.VMEM((GROUPS * WINDOW, L), f32),
        ],
        arrived,
    )
    returned = lax.all_to_all(heads_out, "rows", split_axis=0, concat_axis=0, tiled=True)
    merged, strip = call(
        merge_kernel,
        (shape(W, C, L), shape(3, C, L)),
        [pltpu.VMEM((GROUPS * WINDOW, L), f32), pltpu.VMEM((WIDE, D), f32), pltpu.VMEM((PC * L, D), f32)],
        returned, tokens, low_rim, high_rim, out_weight, unpatch_rows, mixed,
    )
    return call(
        back_kernel,
        jax.ShapeDtypeStruct((C, W, L), bf16),
        [pltpu.VMEM((W + 2, 3 * C, L), bf16), pltpu.VMEM((W, C, L), f32)],
        merged, strip, *exchange(strip, "cols"), conv_out,
    )


def solution(mesh):
    placed = (P(None, "cols", "rows"), P(), P(), P(), P("rows", "cols", None), P(), P(), P())
    return jax.shard_map(
        per_device, mesh=mesh, in_specs=placed, out_specs=P(None, "cols", "rows"), check_vma=False
    )
```

```python
import jax
import jax.numpy as jnp
from jax import lax
from jax.experimental import pallas as pl
from jax.experimental.pallas import tpu as pltpu
from jax.sharding import PartitionSpec as P

C = 32
PATCH = 8
D = 256
HEADS = 8
HEAD_DIM = 32
W = 64
L = 128
PC = W // PATCH
PR = L // PATCH
GROUPS = 64
SEQ = GROUPS * PR
OWN = PR * PC
WIDE = OWN + 2 * PC
WINDOW = 8
QUAD = 4
epsilon = 1e-05

f32 = jnp.float32
bf16 = jnp.bfloat16
NT = (((1,), (1,)), ((), ()))


def iota(shape, dim):
    return lax.broadcasted_iota(jnp.int32, shape, dim)


def one_hot(condition):
    return jnp.where(condition, 1.0, 0.0).astype(bf16)


def column_edges(slab_of, edges_ref):
    lane = iota((C, L), 1)
    edges = jnp.zeros((C, L), f32)
    for w in range(W):
        slab = slab_of(w)
        first = pltpu.roll(slab, w, 1) if w else slab
        last = pltpu.roll(slab, (W + w + 1) % L, 1) if (W + w + 1) % L else slab
        edges = jnp.where(lane == w, first, edges)
        edges = jnp.where(lane == W + w, last, edges)
    edges_ref[...] = edges.astype(bf16)


def turn_kernel(x_ref, turned_ref, edges_ref, ends_ref, turned_f32):
    turned_f32[...] = jnp.swapaxes(x_ref[...].astype(f32), 0, 1)
    turned_ref[...] = turned_f32[...].astype(bf16)
    ends_ref[0] = turned_ref[0]
    ends_ref[1] = turned_ref[W - 1]
    column_edges(lambda w: turned_f32[w], edges_ref)


def weights_kernel(embed_ref, unpatch_ref, embed_out, unpatch_out):
    for source, target in ((embed_ref[...].astype(f32), embed_out), (unpatch_ref[...].astype(f32).T, unpatch_out)):
        turned = jnp.swapaxes(source.reshape(C, PATCH * PATCH, D), 0, 1)
        for i in range(PATCH):
            for j in range(PATCH):
                target[i, j * C : (j + 1) * C, :] = turned[j * PATCH + i].astype(bf16)


def fill_taps(map_ref, strip, even_strip, other_strip, taps):
    lane = iota((C, L), 1)
    outer = strip[2].astype(f32)
    below, above = zip(*(sides("cols", even_strip[n], other_strip[n]) for n in range(3)))
    for w in range(-1, W + 1):
        if w < 0:
            slab, left, right = below[1], below[2][:, L - 1 : L], below[2][:, W - 1 : W]
        elif w == W:
            slab, left, right = above[0], above[2][:, W : W + 1], above[2][:, 0:1]
        else:
            slab = map_ref[w].astype(f32)
            left, right = outer[:, W + w : W + w + 1], outer[:, w : w + 1]
        taps[w + 1, 0:C, :] = jnp.where(lane == 0, left, pltpu.roll(slab, 1, 1)).astype(bf16)
        taps[w + 1, C : 2 * C, :] = slab.astype(bf16)
        taps[w + 1, 2 * C : 3 * C, :] = jnp.where(lane == L - 1, right, pltpu.roll(slab, L - 1, 1)).astype(bf16)


def banded(weight):
    weight = weight.astype(f32)
    rows = []
    for i in range(QUAD):
        pieces = [weight]
        if i:
            pieces.insert(0, jnp.zeros((C, 3 * C * i), f32))
        if i < QUAD - 1:
            pieces.append(jnp.zeros((C, 3 * C * (QUAD - 1 - i)), f32))
        rows.append(jnp.concatenate(pieces, axis=1))
    return jnp.concatenate(rows, axis=0).astype(bf16)


def conv_quad(band, taps, group):
    window = taps[group * QUAD : group * QUAD + QUAD + 2].reshape((QUAD + 2) * 3 * C, L)
    return jnp.dot(band, window, preferred_element_type=f32)


def front_kernel(
    map_ref, strip_ref, even_strip, other_strip, conv_ref, embed_ref, qkv_ref, bias_ref,
    mixed_ref, tokens_ref, packed_ref, rim_ref, taps, gathered, tokens_f32, rim_f32,
):
    fill_taps(map_ref, strip_ref, even_strip, other_strip, taps)
    band = banded(conv_ref[...])
    row = iota((L, L), 0)
    select = one_hot(iota((L, L), 1) == (row % PR) * PATCH + row // PR)
    for p in range(PC):
        for half in range(PATCH // QUAD):
            group = p * (PATCH // QUAD) + half
            value = conv_quad(band, taps, group)
            value = value / (1.0 + jnp.exp(-value))
            for i in range(QUAD):
                w = group * QUAD + i
                cell = taps[w + 1, C : 2 * C, :].astype(f32) + value[i * C : (i + 1) * C]
                mixed_ref[w] = cell.astype(bf16)
        block = mixed_ref[p * PATCH : (p + 1) * PATCH].reshape(PATCH * C, L)
        sorted_cells = lax.dot_general(select, block, NT, preferred_element_type=f32).astype(bf16)
        for i in range(PATCH):
            gathered[p * PR : (p + 1) * PR, i * D : (i + 1) * D] = sorted_cells[i * PR : (i + 1) * PR]
    tokens = jnp.dot(
        gathered[...], embed_ref[...].reshape(PATCH * D, D), preferred_element_type=f32
    ).astype(bf16)
    tokens_ref[...] = tokens
    values = tokens.astype(f32)
    for half in range(2):
        tokens_f32[...] = values[:, half * L : (half + 1) * L]
        for n, r in enumerate((0, PR - 1)):
            at = (2 * half + n) * PC
            rim_f32[at : at + PC, :] = tokens_f32[pl.ds(r, PC, stride=PR), :]
    rim_ref[1] = rim_f32[...].astype(bf16)
    column_edges(lambda w: mixed_ref[w].astype(f32), rim_ref.at[0])
    centered = values - jnp.mean(values, axis=1, keepdims=True)
    spread = jnp.mean(centered * centered, axis=1, keepdims=True)
    normed = (centered * lax.rsqrt(spread + epsilon)).astype(bf16)
    projected = jnp.dot(normed, qkv_ref[...], preferred_element_type=f32)
    bias = bias_ref[...].astype(f32).reshape(PC * HEADS, PR).T
    filler = jnp.zeros((PR * PC, L - 3 * HEAD_DIM - 1), f32)
    for h in range(HEADS):
        pieces = [projected[:, g * D + h * HEAD_DIM : g * D + (h + 1) * HEAD_DIM] for g in range(3)]
        column = [bias[:, p * HEADS + h : p * HEADS + h + 1] for p in range(PC)]
        tile = jnp.concatenate(pieces + [jnp.concatenate(column, axis=0), filler], axis=1).astype(bf16)
        for p in range(PC):
            packed_ref[p * HEADS + h] = tile[p * PR : (p + 1) * PR]


def attention_kernel(packed_ref, out_ref, rows_f32, padded, windows):
    rows = packed_ref[...].reshape(SEQ, L)
    lane = iota((SEQ, L), 1)
    wide = rows.astype(f32)
    rows_f32[...] = pltpu.roll(jnp.where(lane < HEAD_DIM, wide, 0.0), HEAD_DIM, 1)
    pick = one_hot((iota((8, L), 1) == 3 * HEAD_DIM))
    bias = lax.dot_general(pick, rows, NT, preferred_element_type=f32)[0:1]
    values = jnp.where((lane >= 2 * HEAD_DIM) & (lane < 3 * HEAD_DIM), wide, 0.0)
    scale = HEAD_DIM ** (-0.5)
    total = jnp.zeros((SEQ // 4, L), f32)
    for quarter in range(4):
        queries = rows_f32[pl.ds(quarter, SEQ // 4, stride=4), :].astype(bf16)
        scores = lax.dot_general(queries, rows, NT, preferred_element_type=f32) * scale + bias
        peak = jnp.max(scores, axis=1, keepdims=True)
        weights = jnp.exp(scores - peak)
        share = (weights * (1.0 / jnp.sum(weights, axis=1, keepdims=True))).astype(bf16)
        shift = (quarter * HEAD_DIM - 2 * HEAD_DIM) % L
        placed = (pltpu.roll(values, shift, 1) if shift else values).astype(bf16)
        total = total + jnp.dot(share, placed, preferred_element_type=f32)
    pad = jnp.zeros((8, L), f32)
    padded[0:8, :] = pad
    padded[8 : 8 + SEQ // 4, :] = total
    padded[8 + SEQ // 4 :, :] = pad
    for n in range(WINDOW):
        start = 7 + min(n, 5)
        windows[pl.ds(n, GROUPS, stride=WINDOW), :] = padded[pl.ds(start, GROUPS, stride=4), :]
    out_ref[...] = windows[...].reshape(GROUPS, WINDOW, L).astype(bf16)


def merge_kernel(
    returned_ref, tokens_ref, even_rim, other_rim, out_weight_ref, unpatch_ref, mixed_ref,
    merged_ref, strip_ref, returned_f32, rows_f32, repeated,
):
    returned_f32[...] = returned_ref[...].astype(f32).reshape(GROUPS * WINDOW, L)
    for n in range(6):
        heads = [
            returned_f32[pl.ds(h * WINDOW + n, PC, stride=HEADS * WINDOW), :] for h in range(HEADS)
        ]
        for high in {0: (3,), 5: (0,)}.get(n, range(4)):
            line = jnp.concatenate([x[:, high * HEAD_DIM : (high + 1) * HEAD_DIM] for x in heads], axis=1)
            at = {0: OWN, 5: OWN + PC}.get(n, ((n - 1) * 4 + high) * PC)
            rows_f32[at : at + PC, :] = line
    place, source = iota((WIDE, WIDE), 0), iota((WIDE, WIDE), 1)
    order = one_hot(source == jnp.where(place < OWN, (place % PR) * PC + place // PR, place))
    attended = jnp.dot(order, rows_f32[...].astype(bf16), preferred_element_type=f32).astype(bf16)
    low, high = sides("rows", even_rim[1], other_rim[1])
    tokens = jnp.concatenate(
        [
            tokens_ref[...].astype(f32),
            jnp.concatenate([low[PC : 2 * PC], low[3 * PC : 4 * PC]], axis=1),
            jnp.concatenate([high[0:PC], high[2 * PC : 3 * PC]], axis=1),
        ],
        axis=0,
    )
    updated = (
        tokens + jnp.dot(attended, out_weight_ref[...], preferred_element_type=f32)
    ).astype(bf16)
    place, source = iota((L, WIDE), 0), iota((L, WIDE), 1)
    spread = one_hot(source == jnp.where(place < W, OWN + PC + place // PATCH, OWN + place // PATCH - PC))
    near = jnp.dot(spread, updated, preferred_element_type=f32)
    after = iota((L, D), 0) < W
    grown = lax.dot_general(
        unpatch_ref[0], jnp.where(after, near, 0.0).astype(bf16), NT, preferred_element_type=f32
    ) + lax.dot_general(
        unpatch_ref[PATCH - 1], jnp.where(after, 0.0, near).astype(bf16), NT, preferred_element_type=f32
    )
    lane = iota((C, L), 1)
    before, beyond = sides("rows", even_rim[0], other_rim[0])
    outer = jnp.where(lane < W, beyond, before)
    for j in range(PATCH):
        outer = outer + jnp.where(lane % PATCH == j, grown[j * C : (j + 1) * C], 0.0)
    strip_ref[2] = outer.astype(bf16)
    repeat = one_hot(iota((PC * L, WIDE), 0) // PATCH == iota((PC * L, WIDE), 1))
    repeated[...] = jnp.dot(repeat, updated, preferred_element_type=f32)
    inner = iota((L, D), 0) % PATCH
    for p in range(PC):
        block = repeated[p * L : (p + 1) * L, :]
        grown = jnp.zeros((D, L), f32)
        for i in range(PATCH):
            part = jnp.where(inner == i, block, 0.0).astype(bf16)
            grown = grown + lax.dot_general(unpatch_ref[i], part, NT, preferred_element_type=f32)
        cells = mixed_ref[p * PATCH : (p + 1) * PATCH].astype(f32) + grown.reshape(PATCH, C, L)
        merged_ref[p * PATCH : (p + 1) * PATCH] = cells.astype(bf16)
    strip_ref[0] = merged_ref[0]
    strip_ref[1] = merged_ref[W - 1]


def back_kernel(map_ref, strip_ref, even_strip, other_strip, conv_ref, out_ref, taps, result):
    fill_taps(map_ref, strip_ref, even_strip, other_strip, taps)
    band = banded(conv_ref[...])
    for group in range(W // QUAD):
        value = conv_quad(band, taps, group)
        for i in range(QUAD):
            w = group * QUAD + i
            result[w] = taps[w + 1, C : 2 * C, :].astype(f32) + value[i * C : (i + 1) * C]
    out_ref[...] = jnp.swapaxes(result[...], 0, 1).astype(bf16)


def shape(*dims, dtype=bf16):
    return pltpu.VMEM(dims, dtype)


def call(kernel, outs, scratch, *args, flops=0):
    return pl.pallas_call(
        kernel,
        out_shape=outs,
        in_specs=[pl.BlockSpec(memory_space=pltpu.VMEM)] * len(args),
        scratch_shapes=scratch,
        name=kernel.__name__,
        cost_estimate=pl.CostEstimate(flops=flops, transcendentals=0, bytes_accessed=1 << 20),
        compiler_params=pltpu.CompilerParams(vmem_limit_bytes=24 << 20),
    )(*(pltpu.with_memory_space_constraint(x, pltpu.VMEM) for x in args))


def exchange(block, axis):
    count = lax.axis_size(axis)
    swaps = []
    for first in (0, 1):
        pairs = [(i, i + 1) for i in range(first, count - 1, 2)]
        swaps.append(lax.ppermute(block, axis, pairs + [(j, i) for i, j in pairs]))
    return swaps


def sides(axis, even, other):
    odd = lax.axis_index(axis) % 2 == 1
    even, other = even.astype(f32), other.astype(f32)
    return jnp.where(odd, even, other), jnp.where(odd, other, even)


def per_device(pair_map, conv_in, embed_weight, qkv_weight, key_bias, out_weight, unpatch, conv_out):
    turned, edges, ends = call(
        turn_kernel, (shape(W, C, L), shape(C, L), shape(2, C, L)), [pltpu.VMEM((W, C, L), f32)], pair_map
    )
    embed_rows, unpatch_rows = call(
        weights_kernel, (shape(PATCH, D, D), shape(PATCH, D, D)), [], embed_weight, unpatch, flops=1 << 32
    )
    even_row, other_row = exchange(edges, "rows")
    edges, ends, embed_rows, unpatch_rows = lax.optimization_barrier((edges, ends, embed_rows, unpatch_rows))
    odd = lax.axis_index("rows") % 2 == 1
    outer = jnp.where((iota((C, L), 1) < W) == odd, other_row, even_row)
    strip = jnp.concatenate([ends, outer[None]])
    mixed, tokens, packed, rim = call(
        front_kernel,
        (shape(W, C, L), shape(OWN, D), shape(GROUPS, PR, L), shape(2, C, L)),
        [
            pltpu.VMEM((W + 2, 3 * C, L), bf16), pltpu.VMEM((OWN, PATCH * D), bf16),
            pltpu.VMEM((OWN, L), f32), pltpu.VMEM((4 * PC, L), f32),
        ],
        turned, strip, *exchange(strip, "cols"), conv_in, embed_rows, qkv_weight, key_bias.transpose(1, 2, 0),
    )
    even_rim, other_rim = exchange(rim, "rows")
    arrived = lax.all_to_all(packed, "rows", split_axis=0, concat_axis=0, tiled=True)
    heads_out = call(
        attention_kernel,
        shape(GROUPS, WINDOW, L),
        [
            pltpu.VMEM((SEQ, L), f32), pltpu.VMEM((SEQ // 4 + 16, L), f32),
            pltpu.VMEM((GROUPS * WINDOW, L), f32),
        ],
        arrived,
    )
    returned = lax.all_to_all(heads_out, "rows", split_axis=0, concat_axis=0, tiled=True)
    merged, strip = call(
        merge_kernel,
        (shape(W, C, L), shape(3, C, L)),
        [pltpu.VMEM((GROUPS * WINDOW, L), f32), pltpu.VMEM((WIDE, D), f32), pltpu.VMEM((PC * L, D), f32)],
        returned, tokens, even_rim, other_rim, out_weight, unpatch_rows, mixed,
    )
    return call(
        back_kernel,
        jax.ShapeDtypeStruct((C, W, L), bf16),
        [pltpu.VMEM((W + 2, 3 * C, L), bf16), pltpu.VMEM((W, C, L), f32)],
        merged, strip, *exchange(strip, "cols"), conv_out,
    )


def solution(mesh):
    placed = (P(None, "cols", "rows"), P(), P(), P(), P("rows", "cols", None), P(), P(), P())
    return jax.shard_map(
        per_device, mesh=mesh, in_specs=placed, out_specs=P(None, "cols", "rows"), check_vma=False
    )
```

```python
import jax
import jax.numpy as jnp
from jax import lax
from jax.experimental import pallas as pl
from jax.experimental.pallas import tpu as pltpu
from jax.sharding import PartitionSpec as P

C = 32
PATCH = 8
D = 256
HEADS = 8
HEAD_DIM = 32
W = 64
L = 128
PC = W // PATCH
PR = L // PATCH
GROUPS = 64
SEQ = GROUPS * PR
OWN = PR * PC
WIDE = OWN + 2 * PC
WINDOW = 8
QUAD = 4
epsilon = 1e-05
LOG2_E = 1.4426950408889634

f32 = jnp.float32
bf16 = jnp.bfloat16
NT = (((1,), (1,)), ((), ()))


def iota(shape, dim):
    return lax.broadcasted_iota(jnp.int32, shape, dim)


def one_hot(condition):
    return jnp.where(condition, 1.0, 0.0).astype(bf16)


def column_edges(slab_of, edges_ref):
    lane = iota((C, L), 1)
    edges = jnp.zeros((C, L), f32)
    for w in range(W):
        slab = slab_of(w)
        first = pltpu.roll(slab, w, 1) if w else slab
        last = pltpu.roll(slab, (W + w + 1) % L, 1) if (W + w + 1) % L else slab
        edges = jnp.where(lane == w, first, edges)
        edges = jnp.where(lane == W + w, last, edges)
    edges_ref[...] = edges.astype(bf16)


def turn_kernel(x_ref, turned_ref, edges_ref, ends_ref, turned_f32):
    turned_f32[...] = jnp.swapaxes(x_ref[...].astype(f32), 0, 1)
    turned_ref[...] = turned_f32[...].astype(bf16)
    ends_ref[0] = turned_ref[0]
    ends_ref[1] = turned_ref[W - 1]
    column_edges(lambda w: turned_f32[w], edges_ref)


def weights_kernel(embed_ref, unpatch_ref, embed_out, unpatch_out):
    for source, target in ((embed_ref[...].astype(f32), embed_out), (unpatch_ref[...].astype(f32).T, unpatch_out)):
        turned = jnp.swapaxes(source.reshape(C, PATCH * PATCH, D), 0, 1)
        for i in range(PATCH):
            for j in range(PATCH):
                target[i, j * C : (j + 1) * C, :] = turned[j * PATCH + i].astype(bf16)


def fill_taps(map_ref, strip, even_strip, other_strip, taps):
    lane = iota((C, L), 1)
    outer = strip[2].astype(f32)
    below, above = zip(*(sides("cols", even_strip[n], other_strip[n]) for n in range(3)))
    for w in range(-1, W + 1):
        if w < 0:
            slab, left, right = below[1], below[2][:, L - 1 : L], below[2][:, W - 1 : W]
        elif w == W:
            slab, left, right = above[0], above[2][:, W : W + 1], above[2][:, 0:1]
        else:
            slab = map_ref[w].astype(f32)
            left, right = outer[:, W + w : W + w + 1], outer[:, w : w + 1]
        taps[w + 1, 0:C, :] = jnp.where(lane == 0, left, pltpu.roll(slab, 1, 1)).astype(bf16)
        taps[w + 1, C : 2 * C, :] = slab.astype(bf16)
        taps[w + 1, 2 * C : 3 * C, :] = jnp.where(lane == L - 1, right, pltpu.roll(slab, L - 1, 1)).astype(bf16)


def banded(weight):
    weight = weight.astype(f32)
    rows = []
    for i in range(QUAD):
        pieces = [weight]
        if i:
            pieces.insert(0, jnp.zeros((C, 3 * C * i), f32))
        if i < QUAD - 1:
            pieces.append(jnp.zeros((C, 3 * C * (QUAD - 1 - i)), f32))
        rows.append(jnp.concatenate(pieces, axis=1))
    return jnp.concatenate(rows, axis=0).astype(bf16)


def conv_pair(band, taps, group):
    windows = [
        taps[g * QUAD : g * QUAD + QUAD + 2].reshape((QUAD + 2) * 3 * C, L) for g in (group, group + 1)
    ]
    both = jnp.dot(band, jnp.concatenate(windows, axis=1), preferred_element_type=f32)
    return both[:, :L], both[:, L:]


def front_kernel(
    map_ref, strip_ref, even_strip, other_strip, conv_ref, embed_ref, qkv_ref, bias_ref,
    mixed_ref, tokens_ref, packed_ref, rim_ref, taps, gathered, tokens_f32, rim_f32,
):
    fill_taps(map_ref, strip_ref, even_strip, other_strip, taps)
    band = banded(conv_ref[...])
    row = iota((L, L), 0)
    select = one_hot(iota((L, L), 1) == (row % PR) * PATCH + row // PR)
    for p in range(PC):
        group = p * (PATCH // QUAD)
        for half, value in enumerate(conv_pair(band, taps, group)):
            value = value / (1.0 + jnp.exp(-value))
            for i in range(QUAD):
                w = (group + half) * QUAD + i
                cell = taps[w + 1, C : 2 * C, :].astype(f32) + value[i * C : (i + 1) * C]
                mixed_ref[w] = cell.astype(bf16)
        block = mixed_ref[p * PATCH : (p + 1) * PATCH].reshape(PATCH * C, L)
        sorted_cells = lax.dot_general(select, block, NT, preferred_element_type=f32).astype(bf16)
        for i in range(PATCH):
            gathered[p * PR : (p + 1) * PR, i * D : (i + 1) * D] = sorted_cells[i * PR : (i + 1) * PR]
    tokens = jnp.dot(
        gathered[...], embed_ref[...].reshape(PATCH * D, D), preferred_element_type=f32
    ).astype(bf16)
    tokens_ref[...] = tokens
    values = tokens.astype(f32)
    for half in range(2):
        tokens_f32[...] = values[:, half * L : (half + 1) * L]
        for n, r in enumerate((0, PR - 1)):
            at = (2 * half + n) * PC
            rim_f32[at : at + PC, :] = tokens_f32[pl.ds(r, PC, stride=PR), :]
    rim_ref[1] = rim_f32[...].astype(bf16)
    column_edges(lambda w: mixed_ref[w].astype(f32), rim_ref.at[0])
    centered = values - jnp.mean(values, axis=1, keepdims=True)
    spread = jnp.mean(centered * centered, axis=1, keepdims=True)
    normed = (centered * lax.rsqrt(spread + epsilon)).astype(bf16)
    projected = jnp.dot(normed, qkv_ref[...], preferred_element_type=f32)
    bias = bias_ref[...].astype(f32).reshape(PC * HEADS, PR).T
    filler = jnp.zeros((PR * PC, L - 3 * HEAD_DIM - 1), f32)
    for h in range(HEADS):
        pieces = [projected[:, g * D + h * HEAD_DIM : g * D + (h + 1) * HEAD_DIM] for g in range(3)]
        column = [bias[:, p * HEADS + h : p * HEADS + h + 1] for p in range(PC)]
        tile = jnp.concatenate(pieces + [jnp.concatenate(column, axis=0), filler], axis=1).astype(bf16)
        for p in range(PC):
            packed_ref[p * HEADS + h] = tile[p * PR : (p + 1) * PR]


def attention_kernel(packed_ref, out_ref, rows_f32, padded, windows):
    rows = packed_ref[...].reshape(SEQ, L)
    lane = iota((SEQ, L), 1)
    wide = rows.astype(f32)
    rows_f32[...] = pltpu.roll(jnp.where(lane < HEAD_DIM, wide, 0.0), HEAD_DIM, 1)
    pick = one_hot((iota((8, L), 1) == 3 * HEAD_DIM))
    bias = lax.dot_general(pick, rows, NT, preferred_element_type=f32)[0:1]
    values = jnp.where((lane >= 2 * HEAD_DIM) & (lane < 3 * HEAD_DIM), wide, 0.0)
    scale = HEAD_DIM ** (-0.5) * LOG2_E
    bias = bias * LOG2_E
    block_of = iota((SEQ // 4, L), 1) // HEAD_DIM
    total = jnp.zeros((SEQ // 4, L), f32)
    for quarter in range(4):
        queries = rows_f32[pl.ds(quarter, SEQ // 4, stride=4), :].astype(bf16)
        scores = lax.dot_general(queries, rows, NT, preferred_element_type=f32) * scale + bias
        peak = jnp.max(scores, axis=1, keepdims=True)
        weights = jnp.exp2(scores - peak).astype(bf16)
        shift = (quarter * HEAD_DIM - 2 * HEAD_DIM) % L
        placed = pltpu.roll(values, shift, 1) if shift else values
        placed = jnp.where(lane // HEAD_DIM == quarter, placed, 1.0).astype(bf16)
        product = jnp.dot(weights, placed, preferred_element_type=f32)
        sums = pltpu.roll(product, HEAD_DIM, 1)
        total = jnp.where(block_of == quarter, product / sums, total)
    pad = jnp.zeros((8, L), f32)
    padded[0:8, :] = pad
    padded[8 : 8 + SEQ // 4, :] = total
    padded[8 + SEQ // 4 :, :] = pad
    for n in range(WINDOW):
        start = 7 + min(n, 5)
        windows[pl.ds(n, GROUPS, stride=WINDOW), :] = padded[pl.ds(start, GROUPS, stride=4), :]
    out_ref[...] = windows[...].reshape(GROUPS, WINDOW, L).astype(bf16)


def merge_kernel(
    returned_ref, tokens_ref, even_rim, other_rim, out_weight_ref, unpatch_ref, mixed_ref,
    merged_ref, strip_ref, returned_f32, rows_f32, repeated,
):
    returned_f32[...] = returned_ref[...].astype(f32).reshape(GROUPS * WINDOW, L)
    for n in range(6):
        heads = [
            returned_f32[pl.ds(h * WINDOW + n, PC, stride=HEADS * WINDOW), :] for h in range(HEADS)
        ]
        for high in {0: (3,), 5: (0,)}.get(n, range(4)):
            line = jnp.concatenate([x[:, high * HEAD_DIM : (high + 1) * HEAD_DIM] for x in heads], axis=1)
            at = {0: OWN, 5: OWN + PC}.get(n, ((n - 1) * 4 + high) * PC)
            rows_f32[at : at + PC, :] = line
    place, source = iota((WIDE, WIDE), 0), iota((WIDE, WIDE), 1)
    order = one_hot(source == jnp.where(place < OWN, (place % PR) * PC + place // PR, place))
    attended = jnp.dot(order, rows_f32[...].astype(bf16), preferred_element_type=f32).astype(bf16)
    low, high = sides("rows", even_rim[1], other_rim[1])
    tokens = jnp.concatenate(
        [
            tokens_ref[...].astype(f32),
            jnp.concatenate([low[PC : 2 * PC], low[3 * PC : 4 * PC]], axis=1),
            jnp.concatenate([high[0:PC], high[2 * PC : 3 * PC]], axis=1),
        ],
        axis=0,
    )
    updated = (
        tokens + jnp.dot(attended, out_weight_ref[...], preferred_element_type=f32)
    ).astype(bf16)
    place, source = iota((L, WIDE), 0), iota((L, WIDE), 1)
    spread = one_hot(source == jnp.where(place < W, OWN + PC + place // PATCH, OWN + place // PATCH - PC))
    near = jnp.dot(spread, updated, preferred_element_type=f32)
    after = iota((L, D), 0) < W
    grown = lax.dot_general(
        unpatch_ref[0], jnp.where(after, near, 0.0).astype(bf16), NT, preferred_element_type=f32
    ) + lax.dot_general(
        unpatch_ref[PATCH - 1], jnp.where(after, 0.0, near).astype(bf16), NT, preferred_element_type=f32
    )
    lane = iota((C, L), 1)
    before, beyond = sides("rows", even_rim[0], other_rim[0])
    outer = jnp.where(lane < W, beyond, before)
    for j in range(PATCH):
        outer = outer + jnp.where(lane % PATCH == j, grown[j * C : (j + 1) * C], 0.0)
    strip_ref[2] = outer.astype(bf16)
    repeat = one_hot(iota((PC * L, WIDE), 0) // PATCH == iota((PC * L, WIDE), 1))
    repeated[...] = jnp.dot(repeat, updated, preferred_element_type=f32)
    inner = iota((2 * L, D), 0) % PATCH
    for pair in range(PC // 2):
        block = repeated[pair * 2 * L : (pair + 1) * 2 * L, :]
        grown = jnp.zeros((D, 2 * L), f32)
        for i in range(PATCH):
            part = jnp.where(inner == i, block, 0.0).astype(bf16)
            grown = grown + lax.dot_general(unpatch_ref[i], part, NT, preferred_element_type=f32)
        for side in range(2):
            p = pair * 2 + side
            cells = mixed_ref[p * PATCH : (p + 1) * PATCH].astype(f32)
            cells = cells + grown[:, side * L : (side + 1) * L].reshape(PATCH, C, L)
            merged_ref[p * PATCH : (p + 1) * PATCH] = cells.astype(bf16)
    strip_ref[0] = merged_ref[0]
    strip_ref[1] = merged_ref[W - 1]


def back_kernel(map_ref, strip_ref, even_strip, other_strip, conv_ref, out_ref, taps, result, staged, done):
    fill_taps(map_ref, strip_ref, even_strip, other_strip, taps)
    band = banded(conv_ref[...])
    copies = []
    for group in range(0, W // QUAD, 2):
        for half, value in enumerate(conv_pair(band, taps, group)):
            for i in range(QUAD):
                w = (group + half) * QUAD + i
                result[w] = taps[w + 1, C : 2 * C, :].astype(f32) + value[i * C : (i + 1) * C]
        if group % 4 == 2:
            part = group // 4
            columns = slice(part * 2 * PATCH, (part + 1) * 2 * PATCH)
            staged[:, columns, :] = jnp.swapaxes(result[columns], 0, 1).astype(bf16)
            copies.append(
                pltpu.make_async_copy(staged.at[:, columns, :], out_ref.at[:, columns, :], done.at[part])
            )
            copies[-1].start()
    for copy in copies:
        copy.wait()


def shape(*dims, dtype=bf16):
    return pltpu.VMEM(dims, dtype)


def call(kernel, outs, scratch, *args, flops=0, **specs):
    return pl.pallas_call(
        kernel,
        out_shape=outs,
        in_specs=[pl.BlockSpec(memory_space=pltpu.VMEM)] * len(args),
        scratch_shapes=scratch,
        **specs,
        name=kernel.__name__,
        cost_estimate=pl.CostEstimate(flops=flops, transcendentals=0, bytes_accessed=1 << 20),
        compiler_params=pltpu.CompilerParams(vmem_limit_bytes=24 << 20),
    )(*(pltpu.with_memory_space_constraint(x, pltpu.VMEM) for x in args))


def exchange(block, axis):
    count = lax.axis_size(axis)
    swaps = []
    for first in (0, 1):
        pairs = [(i, i + 1) for i in range(first, count - 1, 2)]
        swaps.append(lax.ppermute(block, axis, pairs + [(j, i) for i, j in pairs]))
    return swaps


def sides(axis, even, other):
    odd = lax.axis_index(axis) % 2 == 1
    even, other = even.astype(f32), other.astype(f32)
    return jnp.where(odd, even, other), jnp.where(odd, other, even)


def per_device(pair_map, conv_in, embed_weight, qkv_weight, key_bias, out_weight, unpatch, conv_out):
    turned, edges, ends = call(
        turn_kernel, (shape(W, C, L), shape(C, L), shape(2, C, L)), [pltpu.VMEM((W, C, L), f32)], pair_map
    )
    embed_rows, unpatch_rows = call(
        weights_kernel, (shape(PATCH, D, D), shape(PATCH, D, D)), [], embed_weight, unpatch, flops=1 << 32
    )
    even_row, other_row = exchange(edges, "rows")
    edges, ends, embed_rows, unpatch_rows = lax.optimization_barrier((edges, ends, embed_rows, unpatch_rows))
    odd = lax.axis_index("rows") % 2 == 1
    outer = jnp.where((iota((C, L), 1) < W) == odd, other_row, even_row)
    strip = jnp.concatenate([ends, outer[None]])
    mixed, tokens, packed, rim = call(
        front_kernel,
        (shape(W, C, L), shape(OWN, D), shape(GROUPS, PR, L), shape(2, C, L)),
        [
            pltpu.VMEM((W + 2, 3 * C, L), bf16), pltpu.VMEM((OWN, PATCH * D), bf16),
            pltpu.VMEM((OWN, L), f32), pltpu.VMEM((4 * PC, L), f32),
        ],
        turned, strip, *exchange(strip, "cols"), conv_in, embed_rows, qkv_weight, key_bias.transpose(1, 2, 0),
    )
    even_rim, other_rim = exchange(rim, "rows")
    arrived = lax.all_to_all(packed, "rows", split_axis=0, concat_axis=0, tiled=True)
    heads_out = call(
        attention_kernel,
        shape(GROUPS, WINDOW, L),
        [
            pltpu.VMEM((SEQ, L), f32), pltpu.VMEM((SEQ // 4 + 16, L), f32),
            pltpu.VMEM((GROUPS * WINDOW, L), f32),
        ],
        arrived,
    )
    returned = lax.all_to_all(heads_out, "rows", split_axis=0, concat_axis=0, tiled=True)
    merged, strip = call(
        merge_kernel,
        (shape(W, C, L), shape(3, C, L)),
        [pltpu.VMEM((GROUPS * WINDOW, L), f32), pltpu.VMEM((WIDE, D), f32), pltpu.VMEM((PC * L, D), f32)],
        returned, tokens, even_rim, other_rim, out_weight, unpatch_rows, mixed,
    )
    return call(
        back_kernel,
        jax.ShapeDtypeStruct((C, W, L), bf16),
        [
            pltpu.VMEM((W + 2, 3 * C, L), bf16), pltpu.VMEM((W, C, L), f32),
            pltpu.VMEM((C, W, L), bf16), pltpu.SemaphoreType.DMA((4,)),
        ],
        merged, strip, *exchange(strip, "cols"), conv_out,
        out_specs=pl.BlockSpec(memory_space=pl.ANY),
    )


def solution(mesh):
    placed = (P(None, "cols", "rows"), P(), P(), P(), P("rows", "cols", None), P(), P(), P())
    return jax.shard_map(
        per_device, mesh=mesh, in_specs=placed, out_specs=P(None, "cols", "rows"), check_vma=False
    )
```

```python
import jax
import jax.numpy as jnp
from jax import lax
from jax.experimental import pallas as pl
from jax.experimental.pallas import tpu as pltpu
from jax.sharding import PartitionSpec as P

C = 32
PATCH = 8
D = 256
HEADS = 8
HEAD_DIM = 32
W = 64
L = 128
PC = W // PATCH
PR = L // PATCH
GROUPS = 64
SEQ = GROUPS * PR
OWN = PR * PC
WIDE = OWN + 2 * PC
WINDOW = 8
QUAD = 4
epsilon = 1e-05
LOG2_E = 1.4426950408889634

f32 = jnp.float32
bf16 = jnp.bfloat16
NT = (((1,), (1,)), ((), ()))


def iota(shape, dim):
    return lax.broadcasted_iota(jnp.int32, shape, dim)


def one_hot(condition):
    return jnp.where(condition, 1.0, 0.0).astype(bf16)


def column_edges(slab_of, edges_ref):
    lane = iota((C, L), 1)
    edges = jnp.zeros((C, L), f32)
    for w in range(W):
        slab = slab_of(w)
        first = pltpu.roll(slab, w, 1) if w else slab
        last = pltpu.roll(slab, (W + w + 1) % L, 1) if (W + w + 1) % L else slab
        edges = jnp.where(lane == w, first, edges)
        edges = jnp.where(lane == W + w, last, edges)
    edges_ref[...] = edges.astype(bf16)


def turn_kernel(x_ref, turned_ref, edges_ref, ends_ref, turned_f32):
    turned_f32[...] = jnp.swapaxes(x_ref[...].astype(f32), 0, 1)
    turned_ref[...] = turned_f32[...].astype(bf16)
    ends_ref[0] = turned_ref[0]
    ends_ref[1] = turned_ref[W - 1]
    column_edges(lambda w: turned_f32[w], edges_ref)


def weights_kernel(embed_ref, unpatch_ref, embed_out, unpatch_out):
    for source, target in ((embed_ref[...].astype(f32), embed_out), (unpatch_ref[...].astype(f32).T, unpatch_out)):
        turned = jnp.swapaxes(source.reshape(C, PATCH * PATCH, D), 0, 1)
        for i in range(PATCH):
            for j in range(PATCH):
                target[i, j * C : (j + 1) * C, :] = turned[j * PATCH + i].astype(bf16)


def fill_taps(map_ref, strip, even_strip, other_strip, taps):
    lane = iota((C, L), 1)
    outer = strip[2].astype(f32)
    below, above = zip(*(sides("cols", even_strip[n], other_strip[n]) for n in range(3)))
    for w in range(-1, W + 1):
        if w < 0:
            slab, left, right = below[1], below[2][:, L - 1 : L], below[2][:, W - 1 : W]
        elif w == W:
            slab, left, right = above[0], above[2][:, W : W + 1], above[2][:, 0:1]
        else:
            slab = map_ref[w].astype(f32)
            left, right = outer[:, W + w : W + w + 1], outer[:, w : w + 1]
        taps[w + 1, 0:C, :] = jnp.where(lane == 0, left, pltpu.roll(slab, 1, 1)).astype(bf16)
        taps[w + 1, C : 2 * C, :] = slab.astype(bf16)
        taps[w + 1, 2 * C : 3 * C, :] = jnp.where(lane == L - 1, right, pltpu.roll(slab, L - 1, 1)).astype(bf16)


def banded(weight):
    weight = weight.astype(f32)
    rows = []
    for i in range(QUAD):
        pieces = [weight]
        if i:
            pieces.insert(0, jnp.zeros((C, 3 * C * i), f32))
        if i < QUAD - 1:
            pieces.append(jnp.zeros((C, 3 * C * (QUAD - 1 - i)), f32))
        rows.append(jnp.concatenate(pieces, axis=1))
    return jnp.concatenate(rows, axis=0).astype(bf16)


def conv_pair(band, taps, group):
    windows = [
        taps[g * QUAD : g * QUAD + QUAD + 2].reshape((QUAD + 2) * 3 * C, L) for g in (group, group + 1)
    ]
    both = jnp.dot(band, jnp.concatenate(windows, axis=1), preferred_element_type=f32)
    return both[:, :L], both[:, L:]


def front_kernel(
    map_ref, strip_ref, even_strip, other_strip, conv_ref, embed_ref, qkv_ref, bias_ref,
    mixed_ref, tokens_ref, packed_ref, rim_ref, taps, gathered, tokens_f32, rim_f32,
):
    fill_taps(map_ref, strip_ref, even_strip, other_strip, taps)
    band = banded(conv_ref[...])
    row = iota((L, L), 0)
    select = one_hot(iota((L, L), 1) == (row % PR) * PATCH + row // PR)
    for p in range(PC):
        group = p * (PATCH // QUAD)
        for half, value in enumerate(conv_pair(band, taps, group)):
            value = value / (1.0 + jnp.exp(-value))
            for i in range(QUAD):
                w = (group + half) * QUAD + i
                cell = taps[w + 1, C : 2 * C, :].astype(f32) + value[i * C : (i + 1) * C]
                mixed_ref[w] = cell.astype(bf16)
        block = mixed_ref[p * PATCH : (p + 1) * PATCH].reshape(PATCH * C, L)
        sorted_cells = lax.dot_general(select, block, NT, preferred_element_type=f32).astype(bf16)
        for i in range(PATCH):
            gathered[p * PR : (p + 1) * PR, i * D : (i + 1) * D] = sorted_cells[i * PR : (i + 1) * PR]
    tokens = jnp.dot(
        gathered[...], embed_ref[...].reshape(PATCH * D, D), preferred_element_type=f32
    ).astype(bf16)
    tokens_ref[...] = tokens
    values = tokens.astype(f32)
    for half in range(2):
        tokens_f32[...] = values[:, half * L : (half + 1) * L]
        for n, r in enumerate((0, PR - 1)):
            at = (2 * half + n) * PC
            rim_f32[at : at + PC, :] = tokens_f32[pl.ds(r, PC, stride=PR), :]
    rim_ref[1] = rim_f32[...].astype(bf16)
    column_edges(lambda w: mixed_ref[w].astype(f32), rim_ref.at[0])
    centered = values - jnp.mean(values, axis=1, keepdims=True)
    spread = jnp.mean(centered * centered, axis=1, keepdims=True)
    normed = (centered * lax.rsqrt(spread + epsilon)).astype(bf16)
    projected = jnp.dot(normed, qkv_ref[...], preferred_element_type=f32)
    bias = bias_ref[...].astype(f32).reshape(PC * HEADS, PR).T
    filler = jnp.zeros((PR * PC, L - 3 * HEAD_DIM - 1), f32)
    for h in range(HEADS):
        pieces = [projected[:, g * D + h * HEAD_DIM : g * D + (h + 1) * HEAD_DIM] for g in range(3)]
        column = [bias[:, p * HEADS + h : p * HEADS + h + 1] for p in range(PC)]
        tile = jnp.concatenate(pieces + [jnp.concatenate(column, axis=0), filler], axis=1).astype(bf16)
        for p in range(PC):
            packed_ref[p * HEADS + h] = tile[p * PR : (p + 1) * PR]


def attention_kernel(packed_ref, out_ref, rows_f32, padded, windows):
    rows = packed_ref[...].reshape(SEQ, L)
    lane = iota((SEQ, L), 1)
    wide = rows.astype(f32)
    rows_f32[...] = pltpu.roll(jnp.where(lane < HEAD_DIM, wide, 0.0), HEAD_DIM, 1)
    pick = one_hot((iota((8, L), 1) == 3 * HEAD_DIM))
    bias = lax.dot_general(pick, rows, NT, preferred_element_type=f32)[0:1]
    values = jnp.where((lane >= 2 * HEAD_DIM) & (lane < 3 * HEAD_DIM), wide, 0.0)
    scale = HEAD_DIM ** (-0.5) * LOG2_E
    bias = bias * LOG2_E
    block_of = iota((SEQ // 4, L), 1) // HEAD_DIM
    total = jnp.zeros((SEQ // 4, L), f32)
    for quarter in range(4):
        queries = rows_f32[pl.ds(quarter, SEQ // 4, stride=4), :].astype(bf16)
        scores = lax.dot_general(queries, rows, NT, preferred_element_type=f32) * scale + bias
        peak = jnp.max(scores, axis=1, keepdims=True)
        weights = jnp.exp2(scores - peak).astype(bf16)
        shift = (quarter * HEAD_DIM - 2 * HEAD_DIM) % L
        placed = pltpu.roll(values, shift, 1) if shift else values
        placed = jnp.where(lane // HEAD_DIM == quarter, placed, 1.0).astype(bf16)
        product = jnp.dot(weights, placed, preferred_element_type=f32)
        sums = pltpu.roll(product, HEAD_DIM, 1)
        total = jnp.where(block_of == quarter, product / sums, total)
    pad = jnp.zeros((8, L), f32)
    padded[0:8, :] = pad
    padded[8 : 8 + SEQ // 4, :] = total
    padded[8 + SEQ // 4 :, :] = pad
    for n in range(WINDOW):
        start = 7 + min(n, 5)
        windows[pl.ds(n, GROUPS, stride=WINDOW), :] = padded[pl.ds(start, GROUPS, stride=4), :]
    out_ref[...] = windows[...].reshape(GROUPS, WINDOW, L).astype(bf16)


def merge_kernel(
    returned_ref, tokens_ref, even_rim, other_rim, out_weight_ref, unpatch_ref, mixed_ref,
    merged_ref, strip_ref, returned_f32, rows_f32, repeated,
):
    returned_f32[...] = returned_ref[...].astype(f32).reshape(GROUPS * WINDOW, L)
    for n in range(6):
        heads = [
            returned_f32[pl.ds(h * WINDOW + n, PC, stride=HEADS * WINDOW), :] for h in range(HEADS)
        ]
        for high in {0: (3,), 5: (0,)}.get(n, range(4)):
            line = jnp.concatenate([x[:, high * HEAD_DIM : (high + 1) * HEAD_DIM] for x in heads], axis=1)
            at = {0: OWN, 5: OWN + PC}.get(n, ((n - 1) * 4 + high) * PC)
            rows_f32[at : at + PC, :] = line
    place, source = iota((WIDE, WIDE), 0), iota((WIDE, WIDE), 1)
    order = one_hot(source == jnp.where(place < OWN, (place % PR) * PC + place // PR, place))
    attended = jnp.dot(order, rows_f32[...].astype(bf16), preferred_element_type=f32).astype(bf16)
    low, high = sides("rows", even_rim[1], other_rim[1])
    tokens = jnp.concatenate(
        [
            tokens_ref[...].astype(f32),
            jnp.concatenate([low[PC : 2 * PC], low[3 * PC : 4 * PC]], axis=1),
            jnp.concatenate([high[0:PC], high[2 * PC : 3 * PC]], axis=1),
        ],
        axis=0,
    )
    updated = (
        tokens + jnp.dot(attended, out_weight_ref[...], preferred_element_type=f32)
    ).astype(bf16)
    place, source = iota((L, WIDE), 0), iota((L, WIDE), 1)
    spread = one_hot(source == jnp.where(place < W, OWN + PC + place // PATCH, OWN + place // PATCH - PC))
    near = jnp.dot(spread, updated, preferred_element_type=f32)
    after = iota((L, D), 0) < W
    grown = lax.dot_general(
        unpatch_ref[0], jnp.where(after, near, 0.0).astype(bf16), NT, preferred_element_type=f32
    ) + lax.dot_general(
        unpatch_ref[PATCH - 1], jnp.where(after, 0.0, near).astype(bf16), NT, preferred_element_type=f32
    )
    lane = iota((C, L), 1)
    before, beyond = sides("rows", even_rim[0], other_rim[0])
    outer = jnp.where(lane < W, beyond, before)
    for j in range(PATCH):
        outer = outer + jnp.where(lane % PATCH == j, grown[j * C : (j + 1) * C], 0.0)
    strip_ref[2] = outer.astype(bf16)
    repeat = one_hot(iota((PC * L, WIDE), 0) // PATCH == iota((PC * L, WIDE), 1))
    repeated[...] = jnp.dot(repeat, updated, preferred_element_type=f32)
    inner = iota((2 * L, D), 0) % PATCH
    for pair in range(PC // 2):
        block = repeated[pair * 2 * L : (pair + 1) * 2 * L, :]
        grown = jnp.zeros((D, 2 * L), f32)
        for i in range(PATCH):
            part = jnp.where(inner == i, block, 0.0).astype(bf16)
            grown = grown + lax.dot_general(unpatch_ref[i], part, NT, preferred_element_type=f32)
        for side in range(2):
            p = pair * 2 + side
            cells = mixed_ref[p * PATCH : (p + 1) * PATCH].astype(f32)
            cells = cells + grown[:, side * L : (side + 1) * L].reshape(PATCH, C, L)
            merged_ref[p * PATCH : (p + 1) * PATCH] = cells.astype(bf16)
    strip_ref[0] = merged_ref[0]
    strip_ref[1] = merged_ref[W - 1]


def back_kernel(map_ref, strip_ref, even_strip, other_strip, conv_ref, out_ref, taps, result, staged, done):
    fill_taps(map_ref, strip_ref, even_strip, other_strip, taps)
    band = banded(conv_ref[...])
    copies = []
    for group in range(0, W // QUAD, 2):
        for half, value in enumerate(conv_pair(band, taps, group)):
            for i in range(QUAD):
                w = (group + half) * QUAD + i
                result[w] = taps[w + 1, C : 2 * C, :].astype(f32) + value[i * C : (i + 1) * C]
        if group % 4 == 2:
            part = group // 4
            columns = slice(part * 2 * PATCH, (part + 1) * 2 * PATCH)
            staged[:, columns, :] = jnp.swapaxes(result[columns], 0, 1).astype(bf16)
            copies.append(
                pltpu.make_async_copy(staged.at[:, columns, :], out_ref.at[:, columns, :], done.at[part])
            )
            copies[-1].start()
    for copy in copies:
        copy.wait()


def shape(*dims, dtype=bf16):
    return pltpu.VMEM(dims, dtype)


def call(kernel, outs, scratch, *args, flops=0, **specs):
    return pl.pallas_call(
        kernel,
        out_shape=outs,
        in_specs=[pl.BlockSpec(memory_space=pltpu.VMEM)] * len(args),
        scratch_shapes=scratch,
        **specs,
        name=kernel.__name__,
        cost_estimate=pl.CostEstimate(flops=flops, transcendentals=0, bytes_accessed=1 << 20),
        compiler_params=pltpu.CompilerParams(vmem_limit_bytes=24 << 20),
    )(*(pltpu.with_memory_space_constraint(x, pltpu.VMEM) for x in args))


def exchange(block, axis):
    count = lax.axis_size(axis)
    swaps = []
    for first in (0, 1):
        pairs = [(i, i + 1) for i in range(first, count - 1, 2)]
        swaps.append(lax.ppermute(block, axis, pairs + [(j, i) for i, j in pairs]))
    return swaps


def sides(axis, even, other):
    odd = lax.axis_index(axis) % 2 == 1
    even, other = even.astype(f32), other.astype(f32)
    return jnp.where(odd, even, other), jnp.where(odd, other, even)


def per_device(pair_map, conv_in, embed_weight, qkv_weight, key_bias, out_weight, unpatch, conv_out):
    turned, edges, ends = call(
        turn_kernel, (shape(W, C, L), shape(C, L), shape(2, C, L)), [pltpu.VMEM((W, C, L), f32)], pair_map
    )
    embed_rows, unpatch_rows = call(
        weights_kernel, (shape(PATCH, D, D), shape(PATCH, D, D)), [], embed_weight, unpatch, flops=1 << 32
    )
    even_row, other_row = exchange(edges, "rows")
    edges, ends, embed_rows, unpatch_rows = lax.optimization_barrier((edges, ends, embed_rows, unpatch_rows))
    odd = lax.axis_index("rows") % 2 == 1
    outer = jnp.where((iota((C, L), 1) < W) == odd, other_row, even_row)
    strip = jnp.concatenate([ends, outer[None]])
    mixed, tokens, packed, rim = call(
        front_kernel,
        (shape(W, C, L), shape(OWN, D), shape(GROUPS, PR, L), shape(2, C, L)),
        [
            pltpu.VMEM((W + 2, 3 * C, L), bf16), pltpu.VMEM((OWN, PATCH * D), bf16),
            pltpu.VMEM((OWN, L), f32), pltpu.VMEM((4 * PC, L), f32),
        ],
        turned, strip, *exchange(strip, "cols"), conv_in, embed_rows, qkv_weight, key_bias.transpose(1, 2, 0),
    )
    even_rim, other_rim = exchange(rim, "rows")
    arrived = lax.all_to_all(packed, "rows", split_axis=0, concat_axis=0, tiled=True)
    heads_out = call(
        attention_kernel,
        shape(GROUPS, WINDOW, L),
        [
            pltpu.VMEM((SEQ, L), f32), pltpu.VMEM((SEQ // 4 + 16, L), f32),
            pltpu.VMEM((GROUPS * WINDOW, L), f32),
        ],
        arrived,
    )
    heads_out, even_rim, other_rim = lax.optimization_barrier((heads_out, even_rim, other_rim))
    returned = lax.all_to_all(heads_out, "rows", split_axis=0, concat_axis=0, tiled=True)
    merged, strip = call(
        merge_kernel,
        (shape(W, C, L), shape(3, C, L)),
        [pltpu.VMEM((GROUPS * WINDOW, L), f32), pltpu.VMEM((WIDE, D), f32), pltpu.VMEM((PC * L, D), f32)],
        returned, tokens, even_rim, other_rim, out_weight, unpatch_rows, mixed,
    )
    return call(
        back_kernel,
        jax.ShapeDtypeStruct((C, W, L), bf16),
        [
            pltpu.VMEM((W + 2, 3 * C, L), bf16), pltpu.VMEM((W, C, L), f32),
            pltpu.VMEM((C, W, L), bf16), pltpu.SemaphoreType.DMA((4,)),
        ],
        merged, strip, *exchange(strip, "cols"), conv_out,
        out_specs=pl.BlockSpec(memory_space=pl.ANY),
    )


def solution(mesh):
    placed = (P(None, "cols", "rows"), P(), P(), P(), P("rows", "cols", None), P(), P(), P())
    return jax.shard_map(
        per_device, mesh=mesh, in_specs=placed, out_specs=P(None, "cols", "rows"), check_vma=False
    )
```

```python
import jax
import jax.numpy as jnp
from jax import lax
from jax.experimental import pallas as pl
from jax.experimental.pallas import tpu as pltpu
from jax.sharding import PartitionSpec as P

C = 32
PATCH = 8
D = 256
HEADS = 8
HEAD_DIM = 32
W = 64
L = 128
PC = W // PATCH
PR = L // PATCH
GROUPS = 64
SEQ = GROUPS * PR
OWN = PR * PC
WIDE = OWN + 2 * PC
WINDOW = 8
QUAD = 4
epsilon = 1e-05
LOG2_E = 1.4426950408889634

f32 = jnp.float32
bf16 = jnp.bfloat16
NT = (((1,), (1,)), ((), ()))


def iota(shape, dim):
    return lax.broadcasted_iota(jnp.int32, shape, dim)


def one_hot(condition):
    return jnp.where(condition, 1.0, 0.0).astype(bf16)


def column_edges(slab_of, edges_ref):
    lane = iota((C, L), 1)
    edges = jnp.zeros((C, L), f32)
    for w in range(W):
        slab = slab_of(w)
        first = pltpu.roll(slab, w, 1) if w else slab
        last = pltpu.roll(slab, (W + w + 1) % L, 1) if (W + w + 1) % L else slab
        edges = jnp.where(lane == w, first, edges)
        edges = jnp.where(lane == W + w, last, edges)
    edges_ref[...] = edges.astype(bf16)


def turn_kernel(x_ref, turned_ref, edges_ref, ends_ref, turned_f32):
    turned_f32[...] = jnp.swapaxes(x_ref[...].astype(f32), 0, 1)
    turned_ref[...] = turned_f32[...].astype(bf16)
    ends_ref[0] = turned_ref[0]
    ends_ref[1] = turned_ref[W - 1]
    column_edges(lambda w: turned_f32[w], edges_ref)


def weights_kernel(embed_ref, unpatch_ref, embed_out, unpatch_out):
    for source, target in ((embed_ref[...].astype(f32), embed_out), (unpatch_ref[...].astype(f32).T, unpatch_out)):
        turned = jnp.swapaxes(source.reshape(C, PATCH * PATCH, D), 0, 1)
        for i in range(PATCH):
            for j in range(PATCH):
                target[i, j * C : (j + 1) * C, :] = turned[j * PATCH + i].astype(bf16)


def fill_taps(map_ref, strip, even_strip, other_strip, taps):
    lane = iota((C, L), 1)
    outer = strip[2].astype(f32)
    below, above = zip(*(sides("cols", even_strip[n], other_strip[n]) for n in range(3)))
    for w in range(-1, W + 1):
        if w < 0:
            slab, left, right = below[1], below[2][:, L - 1 : L], below[2][:, W - 1 : W]
        elif w == W:
            slab, left, right = above[0], above[2][:, W : W + 1], above[2][:, 0:1]
        else:
            slab = map_ref[w].astype(f32)
            left, right = outer[:, W + w : W + w + 1], outer[:, w : w + 1]
        taps[w + 1, 0:C, :] = jnp.where(lane == 0, left, pltpu.roll(slab, 1, 1)).astype(bf16)
        taps[w + 1, C : 2 * C, :] = slab.astype(bf16)
        taps[w + 1, 2 * C : 3 * C, :] = jnp.where(lane == L - 1, right, pltpu.roll(slab, L - 1, 1)).astype(bf16)


def banded(weight):
    weight = weight.astype(f32)
    rows = []
    for i in range(QUAD):
        pieces = [weight]
        if i:
            pieces.insert(0, jnp.zeros((C, 3 * C * i), f32))
        if i < QUAD - 1:
            pieces.append(jnp.zeros((C, 3 * C * (QUAD - 1 - i)), f32))
        rows.append(jnp.concatenate(pieces, axis=1))
    return jnp.concatenate(rows, axis=0).astype(bf16)


def conv_pair(band, taps, group):
    windows = [
        taps[g * QUAD : g * QUAD + QUAD + 2].reshape((QUAD + 2) * 3 * C, L) for g in (group, group + 1)
    ]
    both = jnp.dot(band, jnp.concatenate(windows, axis=1), preferred_element_type=f32)
    return both[:, :L], both[:, L:]


def front_kernel(
    map_ref, strip_ref, even_strip, other_strip, conv_ref, embed_ref, qkv_ref, bias_ref,
    mixed_ref, tokens_ref, packed_ref, rim_ref, taps, gathered, tokens_f32, rim_f32,
):
    fill_taps(map_ref, strip_ref, even_strip, other_strip, taps)
    band = banded(conv_ref[...])
    row = iota((L, L), 0)
    select = one_hot(iota((L, L), 1) == (row % PR) * PATCH + row // PR)
    for p in range(PC):
        group = p * (PATCH // QUAD)
        for half, value in enumerate(conv_pair(band, taps, group)):
            value = value / (1.0 + jnp.exp(-value))
            for i in range(QUAD):
                w = (group + half) * QUAD + i
                cell = taps[w + 1, C : 2 * C, :].astype(f32) + value[i * C : (i + 1) * C]
                mixed_ref[w] = cell.astype(bf16)
        block = mixed_ref[p * PATCH : (p + 1) * PATCH].reshape(PATCH * C, L)
        sorted_cells = lax.dot_general(select, block, NT, preferred_element_type=f32).astype(bf16)
        for i in range(PATCH):
            gathered[p * PR : (p + 1) * PR, i * D : (i + 1) * D] = sorted_cells[i * PR : (i + 1) * PR]
    tokens = jnp.dot(
        gathered[...], embed_ref[...].reshape(PATCH * D, D), preferred_element_type=f32
    ).astype(bf16)
    tokens_ref[...] = tokens
    values = tokens.astype(f32)
    for half in range(2):
        tokens_f32[...] = values[:, half * L : (half + 1) * L]
        for n, r in enumerate((0, PR - 1)):
            at = (2 * half + n) * PC
            rim_f32[at : at + PC, :] = tokens_f32[pl.ds(r, PC, stride=PR), :]
    rim_ref[1] = rim_f32[...].astype(bf16)
    column_edges(lambda w: mixed_ref[w].astype(f32), rim_ref.at[0])
    centered = values - jnp.mean(values, axis=1, keepdims=True)
    spread = jnp.mean(centered * centered, axis=1, keepdims=True)
    normed = (centered * lax.rsqrt(spread + epsilon)).astype(bf16)
    projected = jnp.dot(normed, qkv_ref[...], preferred_element_type=f32)
    bias = bias_ref[...].astype(f32).reshape(PC * HEADS, PR).T
    filler = jnp.zeros((PR * PC, L - 3 * HEAD_DIM - 1), f32)
    for h in range(HEADS):
        pieces = [projected[:, g * D + h * HEAD_DIM : g * D + (h + 1) * HEAD_DIM] for g in range(3)]
        column = [bias[:, p * HEADS + h : p * HEADS + h + 1] for p in range(PC)]
        tile = jnp.concatenate(pieces + [jnp.concatenate(column, axis=0), filler], axis=1).astype(bf16)
        for p in range(PC):
            packed_ref[p * HEADS + h] = tile[p * PR : (p + 1) * PR]


def attention_kernel(packed_ref, out_ref, rows_f32, bias_f32, padded, windows):
    rows = packed_ref[...].reshape(SEQ, L)
    wide = rows.astype(f32)
    rows_f32[...] = pltpu.roll(jnp.where(iota((SEQ, L), 1) < HEAD_DIM, wide, 0.0), HEAD_DIM, 1)
    bias_f32[...] = jnp.broadcast_to(wide[:, 3 * HEAD_DIM : 3 * HEAD_DIM + 1] * LOG2_E, (SEQ, L))
    values = jnp.concatenate(
        [wide.T[2 * HEAD_DIM : 3 * HEAD_DIM], jnp.ones((16, SEQ), f32)], axis=0
    ).astype(bf16)
    scale = HEAD_DIM ** (-0.5) * LOG2_E
    quarters = []
    for quarter in range(4):
        queries = rows_f32[pl.ds(quarter, SEQ // 4, stride=4), :].astype(bf16)
        scores = lax.dot_general(rows, queries, NT, preferred_element_type=f32) * scale
        scores = scores + jnp.concatenate([bias_f32[...]] * (SEQ // 4 // L), axis=1)
        weights = jnp.exp2(scores - jnp.max(scores, axis=0, keepdims=True)).astype(bf16)
        product = jnp.dot(values, weights, preferred_element_type=f32)
        quarters.append(product[:HEAD_DIM] / product[HEAD_DIM : HEAD_DIM + 1])
    total = jnp.concatenate(quarters, axis=0).T
    pad = jnp.zeros((8, L), f32)
    padded[0:8, :] = pad
    padded[8 : 8 + SEQ // 4, :] = total
    padded[8 + SEQ // 4 :, :] = pad
    for n in range(WINDOW):
        start = 7 + min(n, 5)
        windows[pl.ds(n, GROUPS, stride=WINDOW), :] = padded[pl.ds(start, GROUPS, stride=4), :]
    out_ref[...] = windows[...].reshape(GROUPS, WINDOW, L).astype(bf16)


def merge_kernel(
    returned_ref, tokens_ref, even_rim, other_rim, out_weight_ref, unpatch_ref, mixed_ref,
    merged_ref, strip_ref, returned_f32, rows_f32, repeated,
):
    returned_f32[...] = returned_ref[...].astype(f32).reshape(GROUPS * WINDOW, L)
    for n in range(6):
        heads = [
            returned_f32[pl.ds(h * WINDOW + n, PC, stride=HEADS * WINDOW), :] for h in range(HEADS)
        ]
        for high in {0: (3,), 5: (0,)}.get(n, range(4)):
            line = jnp.concatenate([x[:, high * HEAD_DIM : (high + 1) * HEAD_DIM] for x in heads], axis=1)
            at = {0: OWN, 5: OWN + PC}.get(n, ((n - 1) * 4 + high) * PC)
            rows_f32[at : at + PC, :] = line
    place, source = iota((WIDE, WIDE), 0), iota((WIDE, WIDE), 1)
    order = one_hot(source == jnp.where(place < OWN, (place % PR) * PC + place // PR, place))
    attended = jnp.dot(order, rows_f32[...].astype(bf16), preferred_element_type=f32).astype(bf16)
    low, high = sides("rows", even_rim[1], other_rim[1])
    tokens = jnp.concatenate(
        [
            tokens_ref[...].astype(f32),
            jnp.concatenate([low[PC : 2 * PC], low[3 * PC : 4 * PC]], axis=1),
            jnp.concatenate([high[0:PC], high[2 * PC : 3 * PC]], axis=1),
        ],
        axis=0,
    )
    updated = (
        tokens + jnp.dot(attended, out_weight_ref[...], preferred_element_type=f32)
    ).astype(bf16)
    place, source = iota((L, WIDE), 0), iota((L, WIDE), 1)
    spread = one_hot(source == jnp.where(place < W, OWN + PC + place // PATCH, OWN + place // PATCH - PC))
    near = jnp.dot(spread, updated, preferred_element_type=f32)
    after = iota((L, D), 0) < W
    grown = lax.dot_general(
        unpatch_ref[0], jnp.where(after, near, 0.0).astype(bf16), NT, preferred_element_type=f32
    ) + lax.dot_general(
        unpatch_ref[PATCH - 1], jnp.where(after, 0.0, near).astype(bf16), NT, preferred_element_type=f32
    )
    lane = iota((C, L), 1)
    before, beyond = sides("rows", even_rim[0], other_rim[0])
    outer = jnp.where(lane < W, beyond, before)
    for j in range(PATCH):
        outer = outer + jnp.where(lane % PATCH == j, grown[j * C : (j + 1) * C], 0.0)
    strip_ref[2] = outer.astype(bf16)
    repeat = one_hot(iota((PC * L, WIDE), 0) // PATCH == iota((PC * L, WIDE), 1))
    repeated[...] = jnp.dot(repeat, updated, preferred_element_type=f32)
    inner = iota((2 * L, D), 0) % PATCH
    for pair in range(PC // 2):
        block = repeated[pair * 2 * L : (pair + 1) * 2 * L, :]
        grown = jnp.zeros((D, 2 * L), f32)
        for i in range(PATCH):
            part = jnp.where(inner == i, block, 0.0).astype(bf16)
            grown = grown + lax.dot_general(unpatch_ref[i], part, NT, preferred_element_type=f32)
        for side in range(2):
            p = pair * 2 + side
            cells = mixed_ref[p * PATCH : (p + 1) * PATCH].astype(f32)
            cells = cells + grown[:, side * L : (side + 1) * L].reshape(PATCH, C, L)
            merged_ref[p * PATCH : (p + 1) * PATCH] = cells.astype(bf16)
    strip_ref[0] = merged_ref[0]
    strip_ref[1] = merged_ref[W - 1]


def back_kernel(map_ref, strip_ref, even_strip, other_strip, conv_ref, out_ref, taps, result, staged, done):
    fill_taps(map_ref, strip_ref, even_strip, other_strip, taps)
    band = banded(conv_ref[...])
    copies = []
    for group in range(0, W // QUAD, 2):
        for half, value in enumerate(conv_pair(band, taps, group)):
            for i in range(QUAD):
                w = (group + half) * QUAD + i
                result[w] = taps[w + 1, C : 2 * C, :].astype(f32) + value[i * C : (i + 1) * C]
        if group % 4 == 2:
            part = group // 4
            columns = slice(part * 2 * PATCH, (part + 1) * 2 * PATCH)
            staged[:, columns, :] = jnp.swapaxes(result[columns], 0, 1).astype(bf16)
            copies.append(
                pltpu.make_async_copy(staged.at[:, columns, :], out_ref.at[:, columns, :], done.at[part])
            )
            copies[-1].start()
    for copy in copies:
        copy.wait()


def shape(*dims, dtype=bf16):
    return pltpu.VMEM(dims, dtype)


def call(kernel, outs, scratch, *args, flops=0, **specs):
    return pl.pallas_call(
        kernel,
        out_shape=outs,
        in_specs=[pl.BlockSpec(memory_space=pltpu.VMEM)] * len(args),
        scratch_shapes=scratch,
        **specs,
        name=kernel.__name__,
        cost_estimate=pl.CostEstimate(flops=flops, transcendentals=0, bytes_accessed=1 << 20),
        compiler_params=pltpu.CompilerParams(vmem_limit_bytes=24 << 20),
    )(*(pltpu.with_memory_space_constraint(x, pltpu.VMEM) for x in args))


def exchange(block, axis):
    count = lax.axis_size(axis)
    swaps = []
    for first in (0, 1):
        pairs = [(i, i + 1) for i in range(first, count - 1, 2)]
        swaps.append(lax.ppermute(block, axis, pairs + [(j, i) for i, j in pairs]))
    return swaps


def sides(axis, even, other):
    odd = lax.axis_index(axis) % 2 == 1
    even, other = even.astype(f32), other.astype(f32)
    return jnp.where(odd, even, other), jnp.where(odd, other, even)


def per_device(pair_map, conv_in, embed_weight, qkv_weight, key_bias, out_weight, unpatch, conv_out):
    turned, edges, ends = call(
        turn_kernel, (shape(W, C, L), shape(C, L), shape(2, C, L)), [pltpu.VMEM((W, C, L), f32)], pair_map
    )
    embed_rows, unpatch_rows = call(
        weights_kernel, (shape(PATCH, D, D), shape(PATCH, D, D)), [], embed_weight, unpatch, flops=1 << 32
    )
    even_row, other_row = exchange(edges, "rows")
    edges, ends, embed_rows, unpatch_rows = lax.optimization_barrier((edges, ends, embed_rows, unpatch_rows))
    odd = lax.axis_index("rows") % 2 == 1
    outer = jnp.where((iota((C, L), 1) < W) == odd, other_row, even_row)
    strip = jnp.concatenate([ends, outer[None]])
    mixed, tokens, packed, rim = call(
        front_kernel,
        (shape(W, C, L), shape(OWN, D), shape(GROUPS, PR, L), shape(2, C, L)),
        [
            pltpu.VMEM((W + 2, 3 * C, L), bf16), pltpu.VMEM((OWN, PATCH * D), bf16),
            pltpu.VMEM((OWN, L), f32), pltpu.VMEM((4 * PC, L), f32),
        ],
        turned, strip, *exchange(strip, "cols"), conv_in, embed_rows, qkv_weight, key_bias.transpose(1, 2, 0),
    )
    even_rim, other_rim = exchange(rim, "rows")
    arrived = lax.all_to_all(packed, "rows", split_axis=0, concat_axis=0, tiled=True)
    heads_out = call(
        attention_kernel,
        shape(GROUPS, WINDOW, L),
        [
            pltpu.VMEM((SEQ, L), f32), pltpu.VMEM((SEQ, L), f32), pltpu.VMEM((SEQ // 4 + 16, L), f32),
            pltpu.VMEM((GROUPS * WINDOW, L), f32),
        ],
        arrived,
    )
    returned = lax.all_to_all(heads_out, "rows", split_axis=0, concat_axis=0, tiled=True)
    merged, strip = call(
        merge_kernel,
        (shape(W, C, L), shape(3, C, L)),
        [pltpu.VMEM((GROUPS * WINDOW, L), f32), pltpu.VMEM((WIDE, D), f32), pltpu.VMEM((PC * L, D), f32)],
        returned, tokens, even_rim, other_rim, out_weight, unpatch_rows, mixed,
    )
    return call(
        back_kernel,
        jax.ShapeDtypeStruct((C, W, L), bf16),
        [
            pltpu.VMEM((W + 2, 3 * C, L), bf16), pltpu.VMEM((W, C, L), f32),
            pltpu.VMEM((C, W, L), bf16), pltpu.SemaphoreType.DMA((4,)),
        ],
        merged, strip, *exchange(strip, "cols"), conv_out,
        out_specs=pl.BlockSpec(memory_space=pl.ANY),
    )


def solution(mesh):
    placed = (P(None, "cols", "rows"), P(), P(), P(), P("rows", "cols", None), P(), P(), P())
    return jax.shard_map(
        per_device, mesh=mesh, in_specs=placed, out_specs=P(None, "cols", "rows"), check_vma=False
    )
```
